8 devices in a mesh: dp: 1 (over z), tp: 2 (over y), sp: 4 (over x, core).
Axes of the slice: x: 2, y: 2, z: 1, core: 2. Of those that a mesh axis runs over, the one named last changes fastest.
Arguments:
- layer_in: bfloat16 [128, 4096], P('dp')
- new_pos: int32 [128], P('dp')
- k_cache: bfloat16 [128, 512, 8, 128], P('dp', 'sp', 'tp')
- v_cache: bfloat16 [128, 512, 8, 128], P('dp', 'sp', 'tp')
- attn_gain: bfloat16 [4096], replicated
- w_query: bfloat16 [4096, 4096], P(None, 'tp')
- w_key: bfloat16 [4096, 1024], P(None, 'tp')
- w_value: bfloat16 [4096, 1024], P(None, 'tp')
- w_out: bfloat16 [4096, 4096], P('tp')
- mlp_gain: bfloat16 [4096], replicated
- w_gate: bfloat16 [4096, 14336], P(None, 'tp')
- w_up: bfloat16 [4096, 14336], P(None, 'tp')
- w_down: bfloat16 [14336, 4096], P('tp')
Outputs:
- output 1: bfloat16 [128, 4096], P('dp')
- output 2: bfloat16 [128, 512, 8, 128], P('dp', 'sp', 'tp')
- output 3: bfloat16 [128, 512, 8, 128], P('dp', 'sp', 'tp')
- output 4: bfloat16 [128, 8, 128], P('dp', 'tp')
- output 5: bfloat16 [128, 8, 128], P('dp', 'tp')
All inputs are finite; a program needn't handle non-finite values.
Results may differ from the reference program's by a relative error of at most 0.00493161.
Values sent between devices are 32-bit elements.
A program may use at most 1.25 GiB of HBM per device.

```python
import jax
import jax.numpy as jnp
from jax import lax

BATCH_ROWS = 128
CACHE_LEN = 512
MODEL_DIM = 4096
NUM_HEADS = 32
KV_HEADS = 8
HEAD_DIM = 128
FFN_DIM = 14336
ROPE_THETA = 1000000
COARSE_GROUPS = 64
GROUP_SIZE = NUM_HEADS // KV_HEADS
SCORE_SCALE = HEAD_DIM ** -0.5
MIN_POS = CACHE_LEN // 16


def weight(key_w, w_shape, fan_in):
    return (jax.random.normal(key_w, w_shape, jnp.float32) * fan_in ** -0.5).astype(jnp.bfloat16)


def setup_inputs(seed: int = 0, part: int = 0) -> dict:
    part_key = jax.random.fold_in(jax.random.key(seed), part)
    row_keys = jax.random.split(part_key, 7)
    w_keys = jax.random.split(jax.random.key(seed + 1), 9)
    layer_in = jax.random.normal(row_keys[0], (BATCH_ROWS, MODEL_DIM), jnp.float32).astype(jnp.bfloat16)
    pos_draw = jax.random.randint(row_keys[1], (BATCH_ROWS,), MIN_POS, CACHE_LEN)
    new_pos = jnp.where(jnp.arange(BATCH_ROWS) == 0, CACHE_LEN - 1, pos_draw).astype(jnp.int32)
    cache_shape = (BATCH_ROWS, CACHE_LEN, KV_HEADS, HEAD_DIM)
    coarse_shape = (BATCH_ROWS, COARSE_GROUPS, 1, KV_HEADS, HEAD_DIM)
    span_shape = (BATCH_ROWS, COARSE_GROUPS, CACHE_LEN // COARSE_GROUPS, KV_HEADS, HEAD_DIM)
    k_coarse = jnp.broadcast_to(jax.random.normal(row_keys[2], coarse_shape, jnp.float32), span_shape).reshape(cache_shape)
    v_coarse = jnp.broadcast_to(jax.random.normal(row_keys[3], coarse_shape, jnp.float32), span_shape).reshape(cache_shape)
    k_cache = (jax.random.normal(row_keys[4], cache_shape, jnp.float32) + 1.5 * k_coarse).astype(jnp.bfloat16)
    v_cache = (0.5 * jax.random.normal(row_keys[5], cache_shape, jnp.float32) + 2.0 * v_coarse).astype(jnp.bfloat16)
    attn_gain = (1.0 + 0.2 * jax.random.normal(w_keys[0], (MODEL_DIM,), jnp.float32)).astype(jnp.bfloat16)
    mlp_gain = (1.0 + 0.2 * jax.random.normal(w_keys[1], (MODEL_DIM,), jnp.float32)).astype(jnp.bfloat16)
    return {
        'layer_in': layer_in,
        'new_pos': new_pos,
        'k_cache': k_cache,
        'v_cache': v_cache,
        'attn_gain': attn_gain,
        'w_query': weight(w_keys[2], (MODEL_DIM, NUM_HEADS * HEAD_DIM), MODEL_DIM),
        'w_key': weight(w_keys[3], (MODEL_DIM, KV_HEADS * HEAD_DIM), MODEL_DIM),
        'w_value': weight(w_keys[4], (MODEL_DIM, KV_HEADS * HEAD_DIM), MODEL_DIM),
        'w_out': weight(w_keys[5], (NUM_HEADS * HEAD_DIM, MODEL_DIM), NUM_HEADS * HEAD_DIM),
        'mlp_gain': mlp_gain,
        'w_gate': weight(w_keys[6], (MODEL_DIM, FFN_DIM), MODEL_DIM),
        'w_up': weight(w_keys[7], (MODEL_DIM, FFN_DIM), MODEL_DIM),
        'w_down': weight(w_keys[8], (FFN_DIM, MODEL_DIM), FFN_DIM),
    }


def rms_norm(in_vec, gain_vec):
    mean_sq = jnp.mean(jnp.square(in_vec), axis=-1, keepdims=True)
    return in_vec * lax.rsqrt(mean_sq + 1e-5) * gain_vec.astype(jnp.float32)


def apply_rotary(in_vec, positions):
    half_idx = jnp.arange(HEAD_DIM // 2, dtype=jnp.float32)
    inv_freq = 1.0 / (ROPE_THETA ** (2.0 * half_idx / HEAD_DIM))
    angles = positions.astype(jnp.float32)[:, None] * inv_freq[None, :]
    cos_a = jnp.cos(angles)[:, None, :]
    sin_a = jnp.sin(angles)[:, None, :]
    pair_view = in_vec.reshape(in_vec.shape[:-1] + (HEAD_DIM // 2, 2))
    even_part = pair_view[..., 0]
    odd_part = pair_view[..., 1]
    rotated = jnp.stack([even_part * cos_a - odd_part * sin_a, even_part * sin_a + odd_part * cos_a], axis=-1)
    return rotated.reshape(in_vec.shape)


def reference(layer_in, new_pos, k_cache, v_cache, attn_gain, w_query, w_key, w_value, w_out, mlp_gain, w_gate, w_up, w_down):
    x_f32 = layer_in.astype(jnp.float32)
    normed = rms_norm(x_f32, attn_gain).astype(jnp.bfloat16)
    q_proj = jnp.dot(normed, w_query, preferred_element_type=jnp.float32).reshape(BATCH_ROWS, NUM_HEADS, HEAD_DIM)
    k_proj = jnp.dot(normed, w_key, preferred_element_type=jnp.float32).reshape(BATCH_ROWS, KV_HEADS, HEAD_DIM)
    v_new = jnp.dot(normed, w_value, preferred_element_type=jnp.float32).reshape(BATCH_ROWS, KV_HEADS, HEAD_DIM).astype(jnp.bfloat16)
    q_rot = apply_rotary(q_proj, new_pos).astype(jnp.bfloat16)
    k_rot = apply_rotary(k_proj, new_pos).astype(jnp.bfloat16)
    slot_ids = jnp.arange(CACHE_LEN)

    def one_row(row_args):
        q_row, k_row, v_row, k_rows, v_rows, pos_row = row_args
        is_new = (slot_ids == pos_row)[:, None, None]
        k_upd = jnp.where(is_new, k_row[None], k_rows)
        v_upd = jnp.where(is_new, v_row[None], v_rows)
        q_grp = q_row.reshape(KV_HEADS, GROUP_SIZE, HEAD_DIM).astype(jnp.float32)
        scores = jnp.einsum('kgd,skd->kgs', q_grp, k_upd.astype(jnp.float32)) * SCORE_SCALE
        scores = jnp.where(slot_ids <= pos_row, scores, -jnp.inf)
        row_max = jnp.max(scores, axis=-1, keepdims=True)
        prob_vals = jnp.exp(scores - row_max)
        denom_sum = jnp.sum(prob_vals, axis=-1)
        weighted = jnp.einsum('kgs,skd->kgd', prob_vals.astype(jnp.bfloat16).astype(jnp.float32), v_upd.astype(jnp.float32))
        attn_row = (weighted / denom_sum[..., None]).reshape(NUM_HEADS * HEAD_DIM)
        return attn_row, k_upd, v_upd

    attn_rows, k_out, v_out = lax.map(one_row, (q_rot, k_rot, v_new, k_cache, v_cache, new_pos))
    attn_vec = attn_rows.astype(jnp.bfloat16)
    hidden = x_f32 + jnp.dot(attn_vec, w_out, preferred_element_type=jnp.float32)
    normed_mlp = rms_norm(hidden, mlp_gain).astype(jnp.bfloat16)
    gate_pre = jnp.dot(normed_mlp, w_gate, preferred_element_type=jnp.float32)
    up_proj = jnp.dot(normed_mlp, w_up, preferred_element_type=jnp.float32)
    act_bf = (jax.nn.silu(gate_pre) * up_proj).astype(jnp.bfloat16)
    layer_out = (hidden + jnp.dot(act_bf, w_down, preferred_element_type=jnp.float32)).astype(jnp.bfloat16)
    return (layer_out, k_out, v_out, k_rot, v_new)
```

```python
import functools

import jax
import jax.numpy as jnp
import numpy as np
from jax import lax
from jax.experimental import pallas as pl
from jax.experimental.pallas import tpu as pltpu
from jax.sharding import PartitionSpec as P

ROPE_THETA = 1000000
MESH = pl.DeviceIdType.MESH
F32 = jnp.float32
BF16 = jnp.bfloat16
MIB = 2**20

ROWS = 128
DIM = 4096
HD = 128
SLOTS = 128
KVH = 4
QH = 16
HID = 7168
HSL = HID // 4
NEG = -1e30

RING = 4
WRING = 3


def rms(x, gain):
    ms = jnp.mean(jnp.square(x), axis=-1, keepdims=True)
    return x * lax.rsqrt(ms + 1e-5) * gain.astype(F32)


def attn_kernel(
    pos_s, x_ref, pos_v, freq_ref, gain_ref, wq, wk, wv, k_in, v_in,
    k_out, v_out, o_out, kn_out, vn_out,
    n_s, wbuf, kbuf, vbuf, qf, kf, vf, kdup, vdup, wsem, isem, osem,
):
    sp = lax.axis_index("sp")
    wsrc = [wk, wv] + [wq.at[:, pl.ds(512 * j, 512)] for j in range(4)]

    def wcopy(j):
        return pltpu.make_async_copy(wsrc[j], wbuf.at[j % WRING], wsem.at[j % WRING])

    def copies_in(i, s):
        rows = pl.ds(i * 16, 16)
        return (
            pltpu.make_async_copy(k_in.at[rows], kbuf.at[s], isem.at[0, s]),
            pltpu.make_async_copy(v_in.at[rows], vbuf.at[s], isem.at[1, s]),
        )

    def copies_out(i, s):
        rows = pl.ds(i * 16, 16)
        return (
            pltpu.make_async_copy(kbuf.at[s], k_out.at[rows], osem.at[0, s]),
            pltpu.make_async_copy(vbuf.at[s], v_out.at[rows], osem.at[1, s]),
        )

    for j in range(WRING):
        wcopy(j).start()
    for i in range(2):
        for c in copies_in(i, i):
            c.start()

    n_s[...] = rms(x_ref[...].astype(F32), gain_ref[...]).astype(BF16)
    ang = pos_v[...].astype(F32) * freq_ref[...]
    lane = lax.broadcasted_iota(jnp.int32, (ROWS, HD), 1)
    even = (lane & 1) == 0
    cosr = jnp.cos(ang)
    sinr = jnp.sin(ang)
    sinr = jnp.where(even, -sinr, sinr)

    def rotate(y):
        swap = jnp.where(even, pltpu.roll(y, HD - 1, 1), pltpu.roll(y, 1, 1))
        return y * cosr + swap * sinr

    for j in range(6):
        wcopy(j).wait()
        y = jnp.dot(n_s[...], wbuf[j % WRING], preferred_element_type=F32)
        if j + WRING < 6:
            wcopy(j + WRING).start()
        for hh in range(4):
            yh = y[:, hh * HD : (hh + 1) * HD]
            if j != 1:
                yh = rotate(yh)
            if j >= 2:
                qf[pl.ds((j - 2) * 4 + hh, ROWS, stride=QH), :] = yh
            else:
                one, dup = (kf, kdup) if j == 0 else (vf, vdup)
                one[pl.ds(hh, ROWS, stride=KVH), :] = yh
                for rep in range(4):
                    dup[pl.ds(rep * KVH + hh, ROWS, stride=16), :] = yh
    kn_out[...] = kf[...].astype(BF16)
    vn_out[...] = vf[...].astype(BF16)

    col = lax.broadcasted_iota(jnp.int32, (QH, SLOTS * KVH), 1)
    hrow = lax.broadcasted_iota(jnp.int32, (QH, SLOTS * KVH), 0)
    head_ok = (col & 3) == (hrow >> 2)
    slot_id = jnp.where(head_ok, col >> 2, jnp.int32(1 << 20))
    r16 = lax.broadcasted_iota(jnp.int32, (16, HD), 0) >> 2
    eye = lax.broadcasted_iota(jnp.int32, (128, 128), 0) == lax.broadcasted_iota(
        jnp.int32, (128, 128), 1
    )

    def block(r, _):
        s = lax.rem(r, RING)
        for c in copies_in(r, s):
            c.wait()

        lims = []
        for b in range(16):
            row = r * 16 + b
            lim = pos_s[row] - sp * SLOTS
            lims.append(lim)
            cl = jnp.clip(lim, 0, SLOTS - 1)
            at = pl.ds(pl.multiple_of((cl >> 2) * 16, 16), 16)
            hit = r16 == jnp.where(lim == cl, cl & 3, -1)
            new = pl.ds(pl.multiple_of(row * 16, 16), 16)
            kbuf[s, b, at, :] = jnp.where(hit, kdup[new, :].astype(BF16), kbuf[s, b, at, :])
            vbuf[s, b, at, :] = jnp.where(hit, vdup[new, :].astype(BF16), vbuf[s, b, at, :])

        for c in copies_out(r, s):
            c.start()

        for half in range(2):
            sc = []
            for b in range(8):
                row = r * 16 + half * 8 + b
                q = qf[pl.ds(pl.multiple_of(row * QH, QH), QH), :].astype(BF16)
                t = lax.dot_general(
                    q, kbuf[s, half * 8 + b], (((1,), (1,)), ((), ())),
                    preferred_element_type=F32,
                )
                sc.append(t)
            ms, ls = [], []
            for b in range(8):
                ok = slot_id <= lims[half * 8 + b]
                t = jnp.where(ok, sc[b] * (HD**-0.5), NEG)
                m = jnp.maximum(jnp.max(t, axis=-1, keepdims=True), NEG * 0.1)
                w = jnp.exp(t - m)
                ms.append(m)
                ls.append(jnp.sum(w, axis=-1, keepdims=True))
                o = jnp.dot(w.astype(BF16), vbuf[s, half * 8 + b], preferred_element_type=F32)
                o_out[r, pl.ds((half * 8 + b) * QH, QH), :] = o
            m = jnp.concatenate(ms, axis=0)
            l = jnp.concatenate(ls, axis=0)
            o_out[r, pl.ds(256 + half, 1), :] = jnp.sum(jnp.where(eye, m, 0.0), axis=0, keepdims=True)
            o_out[r, pl.ds(258 + half, 1), :] = jnp.sum(jnp.where(eye, l, 0.0), axis=0, keepdims=True)

        @pl.when(r + 2 < 8)
        def _():
            s2 = lax.rem(r + 2, RING)

            @pl.when(r >= 2)
            def _():
                for c in copies_out(r - 2, s2):
                    c.wait()

            for c in copies_in(r + 2, s2):
                c.start()

        return 0

    lax.fori_loop(0, 8, block, 0)
    for i in range(4, 8):
        for c in copies_out(i, i % RING):
            c.wait()


def run_attn(pos, x, gain, wq, wk, wv, k_blk, v_blk):
    half_idx = np.arange(HD // 2, dtype=np.float32)
    inv = (1.0 / np.power(np.float32(ROPE_THETA), np.float32(2.0) * half_idx / np.float32(HD))).astype(np.float32)
    freq = jnp.asarray(np.repeat(inv, 2)[None, :])
    vm = pl.BlockSpec(memory_space=pltpu.VMEM)
    hbm = pl.BlockSpec(memory_space=pl.ANY)
    cache = jax.ShapeDtypeStruct((ROWS, SLOTS * KVH, HD), BF16)
    new = jax.ShapeDtypeStruct((ROWS * KVH, HD), BF16)
    return pl.pallas_call(
        attn_kernel,
        name="attn",
        out_shape=[cache, cache, jax.ShapeDtypeStruct((8, 264, 128), F32), new, new],
        in_specs=[pl.BlockSpec(memory_space=pltpu.SMEM), vm, vm, vm, vm] + [hbm] * 5,
        out_specs=[hbm, hbm, vm, vm, vm],
        scratch_shapes=[
            pltpu.VMEM((ROWS, DIM), BF16),
            pltpu.VMEM((WRING, DIM, 512), BF16),
            pltpu.VMEM((RING, 16, SLOTS * KVH, HD), BF16),
            pltpu.VMEM((RING, 16, SLOTS * KVH, HD), BF16),
            pltpu.VMEM((ROWS * QH, HD), F32),
            pltpu.VMEM((ROWS * KVH, HD), F32),
            pltpu.VMEM((ROWS * KVH, HD), F32),
            pltpu.VMEM((ROWS * 16, HD), F32),
            pltpu.VMEM((ROWS * 16, HD), F32),
            pltpu.SemaphoreType.DMA((WRING,)),
            pltpu.SemaphoreType.DMA((2, RING)),
            pltpu.SemaphoreType.DMA((2, RING)),
        ],
        compiler_params=pltpu.CompilerParams(vmem_limit_bytes=56 * MIB),
        cost_estimate=pl.CostEstimate(flops=4 * 10**9, bytes_accessed=92 * 10**6, transcendentals=10**6),
    )(
        pos, x, pos[:, None], freq, gain[None, :], wq, wk, wv,
        k_blk.reshape(ROWS, SLOTS * KVH, HD), v_blk.reshape(ROWS, SLOTS * KVH, HD),
    )


NC = 8
CW = DIM // NC
HC = CW // 2


def tail_kernel(
    o_in, x_in, gain_ref, wo, wg, wu, wd,
    out_ref,
    wo_v, wg_v, wu_v, rb1, ob, rb2, ofin, obf, wp, ry, hs, xs, gat, nbf, act,
    part, rd, r1, r2, gat2, wsem, bsem, ysem, gsem, fsem,
):
    sp = lax.axis_index("sp")
    yi = lax.axis_index("tp")
    dp = lax.axis_index("dp")
    core = lax.rem(sp, 2)
    xi = sp // 2
    dev_c = (dp, yi, sp + 1 - 2 * core)
    dev_x = (dp, yi, lax.rem(sp + 2, 4))
    dev_y = (dp, 1 - yi, sp)
    me = core * 4 + xi * 2 + yi
    me_x = core * 4 + (1 - xi) * 2 + yi
    me_y = core * 4 + xi * 2 + 1 - yi
    me_xy = core * 4 + (1 - xi) * 2 + 1 - yi

    def rc(src, dst, sems, dev):
        return pltpu.make_async_remote_copy(
            src_ref=src, dst_ref=dst, send_sem=sems.at[0], recv_sem=sems.at[1],
            device_id=dev, device_id_type=MESH,
        )

    bar = pltpu.get_barrier_semaphore()
    for dev in (dev_c, dev_x, dev_y):
        pl.semaphore_signal(bar, inc=1, device_id=dev, device_id_type=MESH)
    pl.semaphore_wait(bar, 3)

    b1 = rc(o_in.at[pl.ds(4 * (1 - core), 4)], rb1, bsem.at[0], dev_c)
    b1.start()
    hcols = pl.ds(pl.multiple_of(sp * HSL, 128), HSL)
    hrows = pl.ds(pl.multiple_of(sp * HSL, 128), HSL)
    cx = pltpu.make_async_copy(x_in.at[me], xs, wsem.at[0])
    cwo = pltpu.make_async_copy(wo, wo_v, wsem.at[1])
    cwg = pltpu.make_async_copy(wg.at[:, hcols], wg_v, wsem.at[2])
    cwu = pltpu.make_async_copy(wu.at[:, hcols], wu_v, wsem.at[3])
    cwd = pltpu.make_async_copy(wd.at[hrows], wo_v.at[pl.ds(0, HSL)], wsem.at[4])
    for c in (cx, cwo, cwg, cwu):
        c.start()

    def column(v):
        return jnp.transpose(jnp.broadcast_to(v, (128, 128)))

    def merge(a, b, put, last):
        m1, m2 = a[pl.ds(256, 2), :], b[pl.ds(256, 2), :]
        l1, l2 = a[pl.ds(258, 2), :], b[pl.ds(258, 2), :]
        m = jnp.maximum(m1, m2)
        a1 = jnp.exp(m1 - m)
        a2 = jnp.exp(m2 - m)
        l = a1 * l1 + a2 * l2
        if last:
            a1 = a1 / l
            a2 = a2 / l
        for g in range(2):
            rows = pl.ds(g * 128, 128)
            put(g, column(a1[g : g + 1]) * a[rows, :] + column(a2[g : g + 1]) * b[rows, :])
        return m, l

    b1.wait_recv()

    def first(q):
        dst = ob.at[q]

        def put(g, v):
            dst[pl.ds(g * 128, 128), :] = v

        m, l = merge(o_in.at[4 * core + q], rb1.at[q], put, False)
        dst[pl.ds(256, 2), :] = m
        dst[pl.ds(258, 2), :] = l

    first(2 * (1 - xi))
    first(2 * (1 - xi) + 1)
    b2 = rc(ob.at[pl.ds(2 * (1 - xi), 2)], rb2, bsem.at[1], dev_x)
    b2.start()
    first(2 * xi)
    first(2 * xi + 1)
    b2.wait_recv()
    for q in range(2):

        def put(g, v):
            ofin[pl.ds(q * 256 + g * 128, 128), :] = v

        merge(ob.at[2 * xi + q], rb2.at[q], put, True)
    for h in range(QH):
        obf[:, h * HD : (h + 1) * HD] = ofin[pl.ds(h, 32, stride=QH), :].astype(BF16)

    cwo.wait()
    NY = 4
    YW = DIM // NY
    ycp = []
    for j in range(NY):

        def ostep(i, _):
            cols = pl.ds(pl.multiple_of(j * YW + i * 512, 512), 512)
            v = jnp.dot(obf[...], wo_v[:, cols], preferred_element_type=F32)
            wp[:, :, cols] = v.reshape(2, 16, 512)
            return 0

        lax.fori_loop(0, YW // 512, ostep, 0)
        cols = pl.ds(j * YW, YW)
        c = rc(wp.at[1 - yi, :, cols], ry.at[:, cols], ysem.at[j], dev_y)
        c.start()
        ycp.append(c)
    cwd.start()
    cx.wait()
    for j in range(NY):
        cols = pl.ds(j * YW, YW)
        ycp[j].wait_recv()
        hs[:, cols] = xs[:, cols].astype(F32) + wp[yi, :, cols] + ry[:, cols]
    gat[me] = rms(hs[...], gain_ref[...]).astype(BF16).astype(F32)

    def gather0(buf, c0, w, sems):
        cs = pl.ds(c0, w)
        out = []
        for k, dev in ((0, dev_x), (1, dev_y), (2, dev_c)):
            c = rc(buf.at[me, :, cs], buf.at[me, :, cs], sems.at[k], dev)
            c.start()
            out.append(c)
        return out

    def gather1(buf, c0, w, sems, cps):
        lo, hi, cs = pl.ds(c0, w // 2), pl.ds(c0 + w // 2, w // 2), pl.ds(c0, w)
        cps[0].wait_recv()
        a = rc(buf.at[me_x, :, lo], buf.at[me_x, :, lo], sems.at[3], dev_y)
        a.start()
        b = rc(buf.at[me_x, :, cs], buf.at[me_x, :, cs], sems.at[4], dev_c)
        b.start()
        cps[1].wait_recv()
        c = rc(buf.at[me_y, :, hi], buf.at[me_y, :, hi], sems.at[5], dev_x)
        c.start()
        d = rc(buf.at[me_y, :, cs], buf.at[me_y, :, cs], sems.at[6], dev_c)
        d.start()
        return [a, b, c, d]

    def gather2(buf, c0, w, sems, cps):
        cs = pl.ds(c0, w)
        cps[0].wait_recv()
        cps[2].wait_recv()
        c = rc(buf.at[me_xy, :, cs], buf.at[me_xy, :, cs], sems.at[7], dev_c)
        c.start()
        return [c]

    g0 = gather0(gat, 0, DIM, gsem)
    g1 = gather1(gat, 0, DIM, gsem, g0)
    g2 = gather2(gat, 0, DIM, gsem, g1)
    for c in (g0[2], g1[1], g1[3], g2[0]):
        c.wait_recv()

    def cast(r, _):
        nbf[pl.ds(pl.multiple_of(r * 16, 16), 16), :] = gat[r].astype(BF16)
        return 0

    lax.fori_loop(0, 8, cast, 0)
    cwg.wait()
    cwu.wait()

    def up(i, _):
        cols = pl.ds(pl.multiple_of(i * 256, 256), 256)
        g = jnp.dot(nbf[...], wg_v[:, cols], preferred_element_type=F32)
        u = jnp.dot(nbf[...], wu_v[:, cols], preferred_element_type=F32)
        act[:, cols] = (jax.nn.silu(g) * u).astype(BF16)
        return 0

    lax.fori_loop(0, HSL // 256, up, 0)
    cwd.wait()

    state = [dict() for _ in range(NC)]

    def s0(j):
        cs = pl.ds(j * CW, CW)
        v = jnp.dot(act[...], wo_v[pl.ds(0, HSL), cs], preferred_element_type=F32)
        part[:, :, cs] = v.reshape(8, 16, CW)
        c = rc(part.at[pl.ds(4 * (1 - core), 4), :, cs], rd.at[:, :, cs], fsem.at[j, 8], dev_c)
        c.start()
        state[j]["d"] = c

    def s1(j):
        cs = pl.ds(j * CW, CW)
        state[j]["d"].wait()
        mine = pl.ds(4 * core, 4)
        rd[:, :, cs] = part[mine, :, cs] + rd[:, :, cs]
        if j % 2 == 0:
            c = [rc(rd.at[pl.ds(2 * (1 - xi), 2), :, cs], r1.at[:, :, cs], fsem.at[j, 9], dev_x)]
        else:
            c = [
                rc(rd.at[2 * i + 1 - yi, :, cs], r1.at[i, :, cs], fsem.at[j, 9 + i], dev_y)
                for i in range(2)
            ]
        for k in c:
            k.start()
        state[j]["r"] = c

    def s2(j):
        cs = pl.ds(j * CW, CW)
        for k in state[j]["r"]:
            k.wait_recv()
        if j % 2 == 0:
            for i in range(2):
                r1[i, :, cs] = r1[i, :, cs] + rd[2 * xi + i, :, cs]
            c = rc(r1.at[1 - yi, :, cs], r2.at[:, cs], fsem.at[j, 11], dev_y)
        else:
            for i in range(2):
                r1[i, :, cs] = r1[i, :, cs] + rd[2 * i + yi, :, cs]
            c = rc(r1.at[1 - xi, :, cs], r2.at[:, cs], fsem.at[j, 11], dev_x)
        c.start()
        state[j]["r2"] = c

    def s3(j):
        cs = pl.ds(j * CW, CW)
        state[j]["r2"].wait_recv()
        own = r1[yi, :, cs] if j % 2 == 0 else r1[xi, :, cs]
        y = hs[:, cs] + (own + r2[:, cs])
        gat2[me, :, cs] = y.astype(BF16).astype(F32)
        state[j]["g0"] = gather0(gat2, j * CW, CW, fsem.at[j])

    def s4(j):
        state[j]["g1"] = gather1(gat2, j * CW, CW, fsem.at[j], state[j]["g0"])

    def s5(j):
        state[j]["g2"] = gather2(gat2, j * CW, CW, fsem.at[j], state[j]["g1"])

    def s6(j):
        cs = pl.ds(j * CW, CW)
        st = state[j]
        for c in (st["g0"][2], st["g1"][1], st["g1"][3], st["g2"][0]):
            c.wait_recv()
        out_ref[:, :, cs] = gat2[:, :, cs].astype(BF16)

    stages = (s0, s1, s2, s3, s4, s5, s6)
    for t in range(NC + len(stages) - 1):
        for k, stage in enumerate(stages):
            if 0 <= t - k < NC:
                stage(t - k)

    b1.wait_send()
    b2.wait_send()
    for c in ycp + g0 + g1 + g2:
        c.wait_send()
    for st in state:
        for c in st["r"] + [st["r2"]] + st["g0"] + st["g1"] + st["g2"]:
            c.wait_send()


def run_tail(o_part, x, gain, wo, wg, wu, wd):
    vm = pl.BlockSpec(memory_space=pltpu.VMEM)
    hbm = pl.BlockSpec(memory_space=pl.ANY)
    return pl.pallas_call(
        tail_kernel,
        name="tail",
        out_shape=jax.ShapeDtypeStruct((8, 16, DIM), BF16),
        in_specs=[vm, hbm, vm, hbm, hbm, hbm, hbm],
        out_specs=vm,
        scratch_shapes=[
            pltpu.VMEM((2048, DIM), BF16),
            pltpu.VMEM((DIM, HSL), BF16),
            pltpu.VMEM((DIM, HSL), BF16),
            pltpu.VMEM((4, 264, 128), F32),
            pltpu.VMEM((4, 264, 128), F32),
            pltpu.VMEM((2, 264, 128), F32),
            pltpu.VMEM((512, 128), F32),
            pltpu.VMEM((32, 2048), BF16),
            pltpu.VMEM((2, 16, DIM), F32),
            pltpu.VMEM((16, DIM), F32),
            pltpu.VMEM((16, DIM), F32),
            pltpu.VMEM((16, DIM), BF16),
            pltpu.VMEM((8, 16, DIM), F32),
            pltpu.VMEM((ROWS, DIM), BF16),
            pltpu.VMEM((ROWS, HSL), BF16),
            pltpu.VMEM((8, 16, DIM), F32),
            pltpu.VMEM((4, 16, DIM), F32),
            pltpu.VMEM((2, 16, DIM), F32),
            pltpu.VMEM((16, DIM), F32),
            pltpu.VMEM((8, 16, DIM), F32),
            pltpu.SemaphoreType.DMA((5,)),
            pltpu.SemaphoreType.DMA((2, 2)),
            pltpu.SemaphoreType.DMA((4, 2)),
            pltpu.SemaphoreType.DMA((8, 2)),
            pltpu.SemaphoreType.DMA((NC, 12, 2)),
        ],
        compiler_params=pltpu.CompilerParams(
            collective_id=0, has_side_effects=True, vmem_limit_bytes=67043328
        ),
        cost_estimate=pl.CostEstimate(flops=6 * 10**9, bytes_accessed=62 * 10**6, transcendentals=10**6),
    )(o_part, x.reshape(8, 16, DIM), gain[None, :], wo, wg, wu, wd)


def solution(mesh):
    def local_step(layer_in, new_pos, k_blk, v_blk, attn_gain, w_query, w_key, w_value, w_out, mlp_gain, w_gate, w_up, w_down):
        k_upd, v_upd, o_part, k_new, v_new = run_attn(
            new_pos, layer_in, attn_gain, w_query, w_key, w_value, k_blk, v_blk
        )
        y = run_tail(o_part, layer_in, mlp_gain, w_out, w_gate, w_up, w_down)
        shape = (ROWS, SLOTS, KVH, HD)
        new = (ROWS, KVH, HD)
        return y.reshape(ROWS, DIM), k_upd.reshape(shape), v_upd.reshape(shape), k_new.reshape(new), v_new.reshape(new)

    cache_spec = P('dp', 'sp', 'tp', None)
    new_spec = P('dp', 'tp', None)
    in_specs = (P('dp', None), P('dp'), cache_spec, cache_spec, P(None), P(None, 'tp'), P(None, 'tp'), P(None, 'tp'), P('tp', None), P(None), P(None, 'tp'), P(None, 'tp'), P('tp', None))
    out_specs = (P('dp', None), cache_spec, cache_spec, new_spec, new_spec)
    return jax.shard_map(local_step, mesh=mesh, in_specs=in_specs, out_specs=out_specs, check_vma=False)
```

```python
import functools

import jax
import jax.numpy as jnp
import numpy as np
from jax import lax
from jax.experimental import pallas as pl
from jax.experimental.pallas import tpu as pltpu
from jax.sharding import PartitionSpec as P

ROPE_THETA = 1000000
MESH = pl.DeviceIdType.MESH
F32 = jnp.float32
BF16 = jnp.bfloat16
MIB = 2**20

ROWS = 128
DIM = 4096
HD = 128
SLOTS = 128
KVH = 4
QH = 16
HID = 7168
HSL = HID // 4
NEG = -1e30

RING = 4
WRING = 3


def rms(x, gain_ref):
    ms = jnp.mean(jnp.square(x), axis=-1, keepdims=True)
    gain = gain_ref[...].astype(F32)
    gain = jnp.concatenate([gain[j : j + 1, :] for j in range(DIM // 128)], axis=1)
    return x * lax.rsqrt(ms + 1e-5) * gain


def column(v):
    return jnp.transpose(jnp.broadcast_to(v, (128, 128)))


def attn_kernel(
    pos_s, x_ref, pos_v, freq_ref, gain_ref, wq, wk, wv, k_in, v_in,
    k_out, v_out, o_out, kn_out, vn_out,
    n_s, wbuf, kbuf, vbuf, qf, kf, vf, kdup, vdup, wsem, isem, osem,
):
    sp = lax.axis_index("sp")
    wsrc = [wk, wv] + [wq.at[:, pl.ds(512 * j, 512)] for j in range(4)]

    def wcopy(j):
        return pltpu.make_async_copy(wsrc[j], wbuf.at[j % WRING], wsem.at[j % WRING])

    def copies_in(i, s):
        rows = pl.ds(i * 16, 16)
        return (
            pltpu.make_async_copy(k_in.at[rows], kbuf.at[s], isem.at[0, s]),
            pltpu.make_async_copy(v_in.at[rows], vbuf.at[s], isem.at[1, s]),
        )

    def copies_out(i, s):
        rows = pl.ds(i * 16, 16)
        return (
            pltpu.make_async_copy(kbuf.at[s], k_out.at[rows], osem.at[0, s]),
            pltpu.make_async_copy(vbuf.at[s], v_out.at[rows], osem.at[1, s]),
        )

    for j in range(WRING):
        wcopy(j).start()
    for i in range(2):
        for c in copies_in(i, i):
            c.start()

    n_s[...] = rms(x_ref[...].astype(F32), gain_ref).astype(BF16)
    ang = column(pos_v[...].astype(F32)) * freq_ref[...]
    lane = lax.broadcasted_iota(jnp.int32, (ROWS, HD), 1)
    even = (lane & 1) == 0
    cosr = jnp.cos(ang)
    sinr = jnp.sin(ang)
    sinr = jnp.where(even, -sinr, sinr)

    def rotate(y):
        swap = jnp.where(even, pltpu.roll(y, HD - 1, 1), pltpu.roll(y, 1, 1))
        return y * cosr + swap * sinr

    for j in range(6):
        wcopy(j).wait()
        y = jnp.dot(n_s[...], wbuf[j % WRING], preferred_element_type=F32)
        if j + WRING < 6:
            wcopy(j + WRING).start()
        for hh in range(4):
            yh = y[:, hh * HD : (hh + 1) * HD]
            if j != 1:
                yh = rotate(yh)
            if j >= 2:
                qf[pl.ds((j - 2) * 4 + hh, ROWS, stride=QH), :] = yh
            else:
                one, dup = (kf, kdup) if j == 0 else (vf, vdup)
                one[pl.ds(hh, ROWS, stride=KVH), :] = yh
                for rep in range(4):
                    dup[pl.ds(rep * KVH + hh, ROWS, stride=16), :] = yh
    kn_out[...] = kf[...].astype(BF16)
    vn_out[...] = vf[...].astype(BF16)

    col = lax.broadcasted_iota(jnp.int32, (QH, SLOTS * KVH), 1)
    hrow = lax.broadcasted_iota(jnp.int32, (QH, SLOTS * KVH), 0)
    head_ok = (col & 3) == (hrow >> 2)
    slot_id = jnp.where(head_ok, col >> 2, jnp.int32(1 << 20))
    r16 = lax.broadcasted_iota(jnp.int32, (16, HD), 0) >> 2
    eye = lax.broadcasted_iota(jnp.int32, (128, 128), 0) == lax.broadcasted_iota(
        jnp.int32, (128, 128), 1
    )

    def block(r, _):
        s = lax.rem(r, RING)
        for c in copies_in(r, s):
            c.wait()

        lims = []
        for b in range(16):
            row = r * 16 + b
            lim = pos_s[row] - sp * SLOTS
            lims.append(lim)
            cl = jnp.clip(lim, 0, SLOTS - 1)
            at = pl.ds(pl.multiple_of((cl >> 2) * 16, 16), 16)
            hit = r16 == jnp.where(lim == cl, cl & 3, -1)
            new = pl.ds(pl.multiple_of(row * 16, 16), 16)
            kbuf[s, b, at, :] = jnp.where(hit, kdup[new, :].astype(BF16), kbuf[s, b, at, :])
            vbuf[s, b, at, :] = jnp.where(hit, vdup[new, :].astype(BF16), vbuf[s, b, at, :])

        for c in copies_out(r, s):
            c.start()

        for half in range(2):
            sc = []
            for b in range(8):
                row = r * 16 + half * 8 + b
                q = qf[pl.ds(pl.multiple_of(row * QH, QH), QH), :].astype(BF16)
                t = lax.dot_general(
                    q, kbuf[s, half * 8 + b], (((1,), (1,)), ((), ())),
                    preferred_element_type=F32,
                )
                sc.append(t)
            ms, ls = [], []
            for b in range(8):
                ok = slot_id <= lims[half * 8 + b]
                t = jnp.where(ok, sc[b] * (HD**-0.5), NEG)
                m = jnp.maximum(jnp.max(t, axis=-1, keepdims=True), NEG * 0.1)
                w = jnp.exp(t - m)
                ms.append(m)
                ls.append(jnp.sum(w, axis=-1, keepdims=True))
                o = jnp.dot(w.astype(BF16), vbuf[s, half * 8 + b], preferred_element_type=F32)
                o_out[r, pl.ds((half * 8 + b) * QH, QH), :] = o
            m = jnp.concatenate(ms, axis=0)
            l = jnp.concatenate(ls, axis=0)
            o_out[r, pl.ds(256 + half, 1), :] = jnp.sum(jnp.where(eye, m, 0.0), axis=0, keepdims=True)
            o_out[r, pl.ds(258 + half, 1), :] = jnp.sum(jnp.where(eye, l, 0.0), axis=0, keepdims=True)

        @pl.when(r + 2 < 8)
        def _():
            s2 = lax.rem(r + 2, RING)

            @pl.when(r >= 2)
            def _():
                for c in copies_out(r - 2, s2):
                    c.wait()

            for c in copies_in(r + 2, s2):
                c.start()

        return 0

    lax.fori_loop(0, 8, block, 0)
    for i in range(4, 8):
        for c in copies_out(i, i % RING):
            c.wait()


def run_attn(pos, x, gain, wq, wk, wv, k_blk, v_blk):
    half_idx = np.arange(HD // 2, dtype=np.float32)
    inv = (1.0 / np.power(np.float32(ROPE_THETA), np.float32(2.0) * half_idx / np.float32(HD))).astype(np.float32)
    freq = jnp.asarray(np.repeat(inv, 2)[None, :])
    vm = pl.BlockSpec(memory_space=pltpu.VMEM)
    hbm = pl.BlockSpec(memory_space=pl.ANY)
    cache = jax.ShapeDtypeStruct((ROWS, SLOTS * KVH, HD), BF16)
    new = jax.ShapeDtypeStruct((ROWS * KVH, HD), BF16)
    return pl.pallas_call(
        attn_kernel,
        name="attn",
        out_shape=[cache, cache, jax.ShapeDtypeStruct((8, 264, 128), F32), new, new],
        in_specs=[pl.BlockSpec(memory_space=pltpu.SMEM), vm, vm, vm, vm] + [hbm] * 5,
        out_specs=[hbm, hbm, vm, vm, vm],
        scratch_shapes=[
            pltpu.VMEM((ROWS, DIM), BF16),
            pltpu.VMEM((WRING, DIM, 512), BF16),
            pltpu.VMEM((RING, 16, SLOTS * KVH, HD), BF16),
            pltpu.VMEM((RING, 16, SLOTS * KVH, HD), BF16),
            pltpu.VMEM((ROWS * QH, HD), F32),
            pltpu.VMEM((ROWS * KVH, HD), F32),
            pltpu.VMEM((ROWS * KVH, HD), F32),
            pltpu.VMEM((ROWS * 16, HD), F32),
            pltpu.VMEM((ROWS * 16, HD), F32),
            pltpu.SemaphoreType.DMA((WRING,)),
            pltpu.SemaphoreType.DMA((2, RING)),
            pltpu.SemaphoreType.DMA((2, RING)),
        ],
        compiler_params=pltpu.CompilerParams(vmem_limit_bytes=56 * MIB),
        cost_estimate=pl.CostEstimate(flops=4 * 10**9, bytes_accessed=92 * 10**6, transcendentals=10**6),
    )(
        pos, x, pos[None, :], freq, gain.reshape(32, 128), wq, wk, wv,
        k_blk.reshape(ROWS, SLOTS * KVH, HD), v_blk.reshape(ROWS, SLOTS * KVH, HD),
    )


NG = 4
GW = DIM // NG
NC = 4
CW = DIM // NC
HC = CW // 2


def tail_kernel(
    o_in, x_in, gain_ref, wo, wg, wu, wd,
    out_ref,
    wo_v, wg_v, wu_v, rb1, ob, rb2, ofin, obf, wp, ry, hs, xs, gat, nbf, act,
    part, rd, r1, r2, gat2, wsem, bsem, ysem, gsem, fsem,
):
    sp = lax.axis_index("sp")
    yi = lax.axis_index("tp")
    dp = lax.axis_index("dp")
    core = lax.rem(sp, 2)
    xi = sp // 2
    dev_c = (dp, yi, sp + 1 - 2 * core)
    dev_x = (dp, yi, lax.rem(sp + 2, 4))
    dev_y = (dp, 1 - yi, sp)
    me = core * 4 + xi * 2 + yi
    me_x = core * 4 + (1 - xi) * 2 + yi
    me_y = core * 4 + xi * 2 + 1 - yi
    me_xy = core * 4 + (1 - xi) * 2 + 1 - yi

    def rc(src, dst, sems, dev):
        return pltpu.make_async_remote_copy(
            src_ref=src, dst_ref=dst, send_sem=sems.at[0], recv_sem=sems.at[1],
            device_id=dev, device_id_type=MESH,
        )

    bar = pltpu.get_barrier_semaphore()
    for dev in (dev_c, dev_x, dev_y):
        pl.semaphore_signal(bar, inc=1, device_id=dev, device_id_type=MESH)
    pl.semaphore_wait(bar, 3)

    b1 = rc(o_in.at[pl.ds(4 * (1 - core), 4)], rb1, bsem.at[0], dev_c)
    b1.start()
    hcols = pl.ds(pl.multiple_of(sp * HSL, 128), HSL)
    hrows = pl.ds(pl.multiple_of(sp * HSL, 128), HSL)
    cx = pltpu.make_async_copy(x_in.at[me], xs, wsem.at[0])
    cwo = pltpu.make_async_copy(wo, wo_v, wsem.at[1])
    cwg = pltpu.make_async_copy(wg.at[:, hcols], wg_v, wsem.at[2])
    cwu = pltpu.make_async_copy(wu.at[:, hcols], wu_v, wsem.at[3])
    cwd = pltpu.make_async_copy(wd.at[hrows], wo_v.at[pl.ds(0, HSL)], wsem.at[4])
    for c in (cx, cwo, cwg, cwu):
        c.start()

    def merge(a, b, put, last):
        m1, m2 = a[pl.ds(256, 2), :], b[pl.ds(256, 2), :]
        l1, l2 = a[pl.ds(258, 2), :], b[pl.ds(258, 2), :]
        m = jnp.maximum(m1, m2)
        a1 = jnp.exp(m1 - m)
        a2 = jnp.exp(m2 - m)
        l = a1 * l1 + a2 * l2
        if last:
            a1 = a1 / l
            a2 = a2 / l
        for g in range(2):
            rows = pl.ds(g * 128, 128)
            put(g, column(a1[g : g + 1]) * a[rows, :] + column(a2[g : g + 1]) * b[rows, :])
        return m, l

    b1.wait_recv()

    def first(q):
        dst = ob.at[q]

        def put(g, v):
            dst[pl.ds(g * 128, 128), :] = v

        m, l = merge(o_in.at[4 * core + q], rb1.at[q], put, False)
        dst[pl.ds(256, 2), :] = m
        dst[pl.ds(258, 2), :] = l

    first(2 * (1 - xi))
    first(2 * (1 - xi) + 1)
    b2 = rc(ob.at[pl.ds(2 * (1 - xi), 2)], rb2, bsem.at[1], dev_x)
    b2.start()
    first(2 * xi)
    first(2 * xi + 1)
    b2.wait_recv()
    for q in range(2):

        def put(g, v):
            ofin[pl.ds(q * 256 + g * 128, 128), :] = v

        merge(ob.at[2 * xi + q], rb2.at[q], put, True)
    for h in range(QH):
        obf[:, h * HD : (h + 1) * HD] = ofin[pl.ds(h, 32, stride=QH), :].astype(BF16)

    cwo.wait()
    NY = 2
    YW = DIM // NY
    ycp = []
    for j in range(NY):

        def ostep(i, _):
            cols = pl.ds(pl.multiple_of(j * YW + i * 1024, 1024), 1024)
            v = jnp.dot(obf[...], wo_v[:, cols], preferred_element_type=F32)
            wp[:, :, cols] = v.reshape(2, 16, 1024)
            return 0

        lax.fori_loop(0, YW // 1024, ostep, 0)
        cols = pl.ds(j * YW, YW)
        c = rc(wp.at[1 - yi, :, cols], ry.at[:, cols], ysem.at[j], dev_y)
        c.start()
        ycp.append(c)
    cwd.start()
    cx.wait()
    for j in range(NY):
        cols = pl.ds(j * YW, YW)
        ycp[j].wait_recv()
        hs[:, cols] = xs[:, cols].astype(F32) + wp[yi, :, cols] + ry[:, cols]
    gat[me] = rms(hs[...], gain_ref).astype(BF16).astype(F32)

    def gather0(buf, c0, w, sems):
        cs = pl.ds(c0, w)
        out = []
        for k, dev in ((0, dev_x), (1, dev_y), (2, dev_c)):
            c = rc(buf.at[me, :, cs], buf.at[me, :, cs], sems.at[k], dev)
            c.start()
            out.append(c)
        return out

    def gather1(buf, c0, w, sems, cps):
        lo, hi, cs = pl.ds(c0, w // 2), pl.ds(c0 + w // 2, w // 2), pl.ds(c0, w)
        cps[0].wait_recv()
        a = rc(buf.at[me_x, :, lo], buf.at[me_x, :, lo], sems.at[3], dev_y)
        a.start()
        b = rc(buf.at[me_x, :, cs], buf.at[me_x, :, cs], sems.at[4], dev_c)
        b.start()
        cps[1].wait_recv()
        c = rc(buf.at[me_y, :, hi], buf.at[me_y, :, hi], sems.at[5], dev_x)
        c.start()
        d = rc(buf.at[me_y, :, cs], buf.at[me_y, :, cs], sems.at[6], dev_c)
        d.start()
        return [a, b, c, d]

    def gather2(buf, c0, w, sems, cps):
        cs = pl.ds(c0, w)
        cps[0].wait_recv()
        cps[2].wait_recv()
        c = rc(buf.at[me_xy, :, cs], buf.at[me_xy, :, cs], sems.at[7], dev_c)
        c.start()
        return [c]

    g0 = [gather0(gat, j * GW, GW, gsem.at[j]) for j in range(NG)]
    cwg.wait()
    cwu.wait()
    g1 = [gather1(gat, j * GW, GW, gsem.at[j], g0[j]) for j in range(NG)]
    g2 = []

    def up(j):
        for c in (g0[j][2], g1[j][1], g1[j][3], g2[j][0]):
            c.wait_recv()
        ks = pl.ds(j * GW, GW)
        for r in range(8):
            nbf[pl.ds(r * 16, 16), :] = gat[r, :, ks].astype(BF16)

        def step(i, _):
            for w, base in ((wg_v, 0), (wu_v, HSL)):
                v = jnp.dot(
                    nbf[...], w[ks, pl.ds(pl.multiple_of(i * 256, 256), 256)], preferred_element_type=F32
                ).reshape(8, 16, 256)
                cols = pl.ds(pl.multiple_of(base + i * 256, 256), 256)
                part[:, :, cols] = v if j == 0 else part[:, :, cols] + v
            return 0

        lax.fori_loop(0, HSL // 256, step, 0)

    for j in range(NG):
        g2.append(gather2(gat, j * GW, GW, gsem.at[j], g1[j]))
        if j:
            up(j - 1)
    up(NG - 1)

    def gate(i, _):
        cols = pl.ds(pl.multiple_of(i * 256, 256), 256)
        g = part[:, :, cols].reshape(ROWS, 256)
        u = part[:, :, pl.ds(pl.multiple_of(HSL + i * 256, 256), 256)].reshape(ROWS, 256)
        act[:, cols] = (jax.nn.silu(g) * u).astype(BF16)
        return 0

    lax.fori_loop(0, HSL // 256, gate, 0)
    cwd.wait()

    state = [dict() for _ in range(NC)]

    def s0(j):
        cs = pl.ds(j * CW, CW)
        v = jnp.dot(act[...], wo_v[pl.ds(0, HSL), cs], preferred_element_type=F32)
        part[:, :, cs] = v.reshape(8, 16, CW)
        c = rc(part.at[pl.ds(4 * (1 - core), 4), :, cs], rd.at[:, :, cs], fsem.at[j, 8], dev_c)
        c.start()
        state[j]["d"] = c

    def s1(j):
        cs = pl.ds(j * CW, CW)
        state[j]["d"].wait()
        mine = pl.ds(4 * core, 4)
        rd[:, :, cs] = part[mine, :, cs] + rd[:, :, cs]
        if j % 2 == 0:
            c = [rc(rd.at[pl.ds(2 * (1 - xi), 2), :, cs], r1.at[:, :, cs], fsem.at[j, 9], dev_x)]
        else:
            c = [
                rc(rd.at[2 * i + 1 - yi, :, cs], r1.at[i, :, cs], fsem.at[j, 9 + i], dev_y)
                for i in range(2)
            ]
        for k in c:
            k.start()
        state[j]["r"] = c

    def s2(j):
        cs = pl.ds(j * CW, CW)
        for k in state[j]["r"]:
            k.wait_recv()
        if j % 2 == 0:
            for i in range(2):
                r1[i, :, cs] = r1[i, :, cs] + rd[2 * xi + i, :, cs]
            c = rc(r1.at[1 - yi, :, cs], r2.at[:, cs], fsem.at[j, 11], dev_y)
        else:
            for i in range(2):
                r1[i, :, cs] = r1[i, :, cs] + rd[2 * i + yi, :, cs]
            c = rc(r1.at[1 - xi, :, cs], r2.at[:, cs], fsem.at[j, 11], dev_x)
        c.start()
        state[j]["r2"] = c

    def s3(j):
        cs = pl.ds(j * CW, CW)
        state[j]["r2"].wait_recv()
        own = r1[yi, :, cs] if j % 2 == 0 else r1[xi, :, cs]
        y = hs[:, cs] + (own + r2[:, cs])
        gat2[me, :, cs] = y.astype(BF16).astype(F32)
        state[j]["g0"] = gather0(gat2, j * CW, CW, fsem.at[j])

    def s4(j):
        state[j]["g1"] = gather1(gat2, j * CW, CW, fsem.at[j], state[j]["g0"])

    def s5(j):
        state[j]["g2"] = gather2(gat2, j * CW, CW, fsem.at[j], state[j]["g1"])

    def s6(j):
        cs = pl.ds(j * CW, CW)
        st = state[j]
        for c in (st["g0"][2], st["g1"][1], st["g1"][3], st["g2"][0]):
            c.wait_recv()
        out_ref[:, :, cs] = gat2[:, :, cs].astype(BF16)

    for t in range(NC + 1):
        if t < NC:
            s0(t)
        if t:
            s1(t - 1)
    for stage in (s2, s3, s4, s5, s6):
        for j in range(NC):
            stage(j)

    b1.wait_send()
    b2.wait_send()
    for c in ycp + sum(g0 + g1 + g2, []):
        c.wait_send()
    for st in state:
        for c in st["r"] + [st["r2"]] + st["g0"] + st["g1"] + st["g2"]:
            c.wait_send()


def run_tail(o_part, x, gain, wo, wg, wu, wd):
    vm = pl.BlockSpec(memory_space=pltpu.VMEM)
    hbm = pl.BlockSpec(memory_space=pl.ANY)
    return pl.pallas_call(
        tail_kernel,
        name="tail",
        out_shape=jax.ShapeDtypeStruct((8, 16, DIM), BF16),
        in_specs=[vm, hbm, vm, hbm, hbm, hbm, hbm],
        out_specs=vm,
        scratch_shapes=[
            pltpu.VMEM((2048, DIM), BF16),
            pltpu.VMEM((DIM, HSL), BF16),
            pltpu.VMEM((DIM, HSL), BF16),
            pltpu.VMEM((4, 264, 128), F32),
            pltpu.VMEM((4, 264, 128), F32),
            pltpu.VMEM((2, 264, 128), F32),
            pltpu.VMEM((512, 128), F32),
            pltpu.VMEM((32, 2048), BF16),
            pltpu.VMEM((2, 16, DIM), F32),
            pltpu.VMEM((16, DIM), F32),
            pltpu.VMEM((16, DIM), F32),
            pltpu.VMEM((16, DIM), BF16),
            pltpu.VMEM((8, 16, DIM), F32),
            pltpu.VMEM((ROWS, GW), BF16),
            pltpu.VMEM((ROWS, HSL), BF16),
            pltpu.VMEM((8, 16, DIM), F32),
            pltpu.VMEM((4, 16, DIM), F32),
            pltpu.VMEM((2, 16, DIM), F32),
            pltpu.VMEM((16, DIM), F32),
            pltpu.VMEM((8, 16, DIM), F32),
            pltpu.SemaphoreType.DMA((5,)),
            pltpu.SemaphoreType.DMA((2, 2)),
            pltpu.SemaphoreType.DMA((2, 2)),
            pltpu.SemaphoreType.DMA((NG, 8, 2)),
            pltpu.SemaphoreType.DMA((NC, 12, 2)),
        ],
        compiler_params=pltpu.CompilerParams(
            collective_id=0, has_side_effects=True, vmem_limit_bytes=67043328
        ),
        cost_estimate=pl.CostEstimate(flops=6 * 10**9, bytes_accessed=62 * 10**6, transcendentals=10**6),
    )(o_part, x.reshape(8, 16, DIM), gain.reshape(32, 128), wo, wg, wu, wd)


def solution(mesh):
    def local_step(layer_in, new_pos, k_blk, v_blk, attn_gain, w_query, w_key, w_value, w_out, mlp_gain, w_gate, w_up, w_down):
        k_upd, v_upd, o_part, k_new, v_new = run_attn(
            new_pos, layer_in, attn_gain, w_query, w_key, w_value, k_blk, v_blk
        )
        y = run_tail(o_part, layer_in, mlp_gain, w_out, w_gate, w_up, w_down)
        shape = (ROWS, SLOTS, KVH, HD)
        new = (ROWS, KVH, HD)
        return y.reshape(ROWS, DIM), k_upd.reshape(shape), v_upd.reshape(shape), k_new.reshape(new), v_new.reshape(new)

    cache_spec = P('dp', 'sp', 'tp', None)
    new_spec = P('dp', 'tp', None)
    in_specs = (P('dp', None), P('dp'), cache_spec, cache_spec, P(None), P(None, 'tp'), P(None, 'tp'), P(None, 'tp'), P('tp', None), P(None), P(None, 'tp'), P(None, 'tp'), P('tp', None))
    out_specs = (P('dp', None), cache_spec, cache_spec, new_spec, new_spec)
    return jax.shard_map(local_step, mesh=mesh, in_specs=in_specs, out_specs=out_specs, check_vma=False)
```

```python
import functools

import jax
import jax.numpy as jnp
import numpy as np
from jax import lax
from jax.experimental import pallas as pl
from jax.experimental.pallas import tpu as pltpu
from jax.sharding import PartitionSpec as P

ROPE_THETA = 1000000
MESH = pl.DeviceIdType.MESH
F32 = jnp.float32
BF16 = jnp.bfloat16
MIB = 2**20

ROWS = 128
DIM = 4096
HD = 128
SLOTS = 128
KVH = 4
QH = 16
HID = 7168
HSL = HID // 4
NEG = -1e30
PAIR = 2
M_AT = pl.ds(256, PAIR)
L_AT = pl.ds(258, PAIR)
RING = 4

def rms(x, gain_ref):
    ms = jnp.mean(jnp.square(x), axis=-1, keepdims=True)
    gain = gain_ref[...].astype(F32)
    gain = jnp.concatenate([gain[j : j + 1, :] for j in range(DIM // 128)], axis=1)
    return x * lax.rsqrt(ms + 1e-5) * gain


def column(v):
    return jnp.transpose(jnp.broadcast_to(v, (128, 128)))


def place():
    sp = lax.axis_index("sp")
    yi = lax.axis_index("tp")
    dp = lax.axis_index("dp")
    core = lax.rem(sp, 2)
    xi = sp // 2
    oc = 1 - core
    ox = 1 - xi
    return sp, yi, core, xi, oc, ox, (dp, yi, 2 * xi + oc), (dp, yi, 2 * ox + core), (dp, 1 - yi, sp)


def block_of(c, x, y):
    return 4 * c + 2 * x + y


def rc(src, dst, sems, dev):
    return pltpu.make_async_remote_copy(
        src_ref=src, dst_ref=dst, send_sem=sems.at[0], recv_sem=sems.at[1],
        device_id=dev, device_id_type=MESH,
    )


def front_kernel(
    pos_s, x_ref, pos_v, freq_ref, gain_ref, wq, wk, wv, wo, k_in, v_in,
    kn_out, vn_out, kdup, vdup, own_out, oth_out,
    n_s, wbuf, kbuf, vbuf, qraw, kvraw, qf, slotb, o_s, rba, rbb, rbx, ob, ofin, obf,
    wsem, isem, qsem, bsem,
):
    sp, yi, core, xi, oc, ox, dev_c, dev_x, dev_y = place()

    bar = pltpu.get_barrier_semaphore()
    for dev in (dev_c, dev_x):
        pl.semaphore_signal(bar, inc=1, device_id=dev, device_id_type=MESH)

    def row_block(t):
        p, y = t // 2, t % 2
        c = core + (oc - core) * (1 - p % 2)
        x = xi + (ox - xi) * (1 - p // 2)
        return block_of(c, x, y)

    def cache_copies(t):
        rows = pl.ds(row_block(t) * 16, 16)
        return (
            pltpu.make_async_copy(k_in.at[rows], kbuf.at[t % RING], isem.at[0, t % RING]),
            pltpu.make_async_copy(v_in.at[rows], vbuf.at[t % RING], isem.at[1, t % RING]),
        )

    def cols(start, width):
        return pl.ds(pl.multiple_of(start, 128), width)

    wcp = [
        [
            pltpu.make_async_copy(wk.at[:, cols(core * 256, 256)], wbuf.at[0, :, pl.ds(0, 256)], wsem.at[0]),
            pltpu.make_async_copy(wv.at[:, cols(core * 256, 256)], wbuf.at[0, :, pl.ds(256, 256)], wsem.at[1]),
        ],
        [pltpu.make_async_copy(wq.at[:, cols(core * 1024, 512)], wbuf.at[1], wsem.at[2])],
        [pltpu.make_async_copy(wq.at[:, cols(core * 1024 + 512, 512)], wbuf.at[2], wsem.at[3])],
    ]
    ocp = [
        pltpu.make_async_copy(
            wo.at[:, pl.ds(512 * i, 512)], wbuf.at[i // 2, pl.ds(2048 * (i % 2), 2048)], wsem.at[4 + i]
        )
        for i in range(8)
    ]
    for group in wcp:
        for c in group:
            c.start()
    for c in cache_copies(0):
        c.start()

    n_s[...] = rms(x_ref[...].astype(F32), gain_ref).astype(BF16)
    ang = column(pos_v[...].astype(F32)) * freq_ref[...]
    lane = lax.broadcasted_iota(jnp.int32, (ROWS, HD), 1)
    even = (lane & 1) == 0
    cosr = jnp.cos(ang)
    sinr = jnp.sin(ang)
    sinr = jnp.where(even, -sinr, sinr)
    slotb[...] = (lax.broadcasted_iota(jnp.int32, (SLOTS * KVH, HD), 0) >> 2).astype(F32).astype(BF16)

    def rotate(y):
        swap = jnp.where(even, pltpu.roll(y, HD - 1, 1), pltpu.roll(y, 1, 1))
        return y * cosr + swap * sinr

    qcp = []
    for j in range(3):
        for c in wcp[j]:
            c.wait()
        y = jnp.dot(n_s[...], wbuf[j], preferred_element_type=F32)
        for c in cache_copies(1 + j):
            c.start()
        for hh in range(4):
            yh = y[:, hh * HD : (hh + 1) * HD]
            if j == 0 and hh < 2:
                kvraw[0, 2 * core + hh] = rotate(yh)
            elif j == 0:
                kvraw[1, 2 * core + hh - 2] = yh
            else:
                qraw[8 * core + (j - 1) * 4 + hh] = rotate(yh)
        if j == 0:
            pl.semaphore_wait(bar, 2)
            for i in range(PAIR):
                ref = kvraw.at[i, pl.ds(2 * core, 2)]
                qcp.append(rc(ref, ref, qsem.at[i], dev_c))
        else:
            ref = qraw.at[pl.ds(8 * core + (j - 1) * 4, 4)]
            qcp.append(rc(ref, ref, qsem.at[1 + j], dev_c))
            if j == 1:
                qcp[0].start()
                qcp[1].start()
                qcp[2].start()
            else:
                qcp[3].start()
    for c in qcp:
        c.wait_recv()
    for i, (dup, out) in enumerate(((kdup, kn_out), (vdup, vn_out))):
        for h in range(KVH):
            v = kvraw[i, h]
            ofin[pl.ds(h, ROWS, stride=KVH), :] = v
            for rep in range(PAIR):
                dup[pl.ds(rep * KVH + h, ROWS, stride=8), :] = v
        out[...] = ofin[...].astype(BF16)
    for h in range(QH):
        qf[pl.ds(h, ROWS, stride=QH), :] = qraw[h]

    col = lax.broadcasted_iota(jnp.int32, (QH, SLOTS * KVH), 1)
    hrow = lax.broadcasted_iota(jnp.int32, (QH, SLOTS * KVH), 0)
    slot_id = jnp.where((col & 3) == (hrow >> 2), col >> 2, jnp.int32(1 << 20))
    eye = lax.broadcasted_iota(jnp.int32, (128, 128), 0) == lax.broadcasted_iota(
        jnp.int32, (128, 128), 1
    )

    def merge(a, b, put, last):
        m1, m2 = a[M_AT, :], b[M_AT, :]
        l1, l2 = a[L_AT, :], b[L_AT, :]
        m = jnp.maximum(m1, m2)
        a1 = jnp.exp(m1 - m)
        a2 = jnp.exp(m2 - m)
        l = a1 * l1 + a2 * l2
        if last:
            a1 = a1 / l
            a2 = a2 / l
        for g in range(PAIR):
            rows = pl.ds(g * 128, 128)
            put(g, column(a1[g : g + 1]) * a[rows, :] + column(a2[g : g + 1]) * b[rows, :])
        return m, l

    def merge_into(dst, a, b):
        def put(g, v):
            dst[pl.ds(g * 128, 128), :] = v

        m, l = merge(a, b, put, False)
        dst[M_AT, :] = m
        dst[L_AT, :] = l

    pair = {
        "a": block_of(oc, ox, 0),
        "x": block_of(core, ox, 0),
        "b": block_of(oc, xi, 0),
        "own": block_of(core, xi, 0),
    }
    send_a = rc(o_s.at[pl.ds(pair["a"], 2)], rba, bsem.at[0], dev_c)
    send_b = rc(o_s.at[pl.ds(pair["b"], 2)], rbb, bsem.at[1], dev_c)
    send_x = rc(ob.at[pl.ds(0, 2)], rbx, bsem.at[2], dev_x)

    def block(t, _):
        r = row_block(t)
        for c in cache_copies(t):
            c.wait()

        @pl.when(t == 4)
        def _():
            for c in ocp:
                c.start()

        for half in range(PAIR):
            sc, lims, vals = [], [], []
            for b in range(8):
                row = r * 16 + half * 8 + b
                lim = pos_s[row] - sp * SLOTS
                lims.append(lim)
                hit = slotb[...] == lax.broadcast(lim.astype(F32), (SLOTS * KVH, HD)).astype(BF16)
                new = pl.ds(pl.multiple_of(row * 8, 8), 8)
                kv = []
                for dup, ref in ((kdup, kbuf), (vdup, vbuf)):
                    d = dup[new, :]
                    d = jnp.concatenate([d, d], axis=0).astype(BF16)
                    d = jnp.concatenate([d] * 32, axis=0)
                    kv.append(jnp.where(hit, d, ref[t % RING, half * 8 + b]))
                vals.append(kv[1])
                q = qf[pl.ds(pl.multiple_of(row * QH, QH), QH), :].astype(BF16)
                sc.append(
                    lax.dot_general(
                        q, kv[0], (((1,), (1,)), ((), ())), preferred_element_type=F32
                    )
                )
            ms, ls = [], []
            for b in range(8):
                ok = slot_id <= lims[b]
                s = jnp.where(ok, sc[b] * (HD**-0.5), NEG)
                m = jnp.maximum(jnp.max(s, axis=-1, keepdims=True), NEG * 0.1)
                w = jnp.exp(s - m)
                ms.append(m)
                ls.append(jnp.sum(w, axis=-1, keepdims=True))
                o = jnp.dot(w.astype(BF16), vals[b], preferred_element_type=F32)
                o_s[r, pl.ds((half * 8 + b) * QH, QH), :] = o
            m = jnp.concatenate(ms, axis=0)
            l = jnp.concatenate(ls, axis=0)
            o_s[r, pl.ds(256 + half, 1), :] = jnp.sum(jnp.where(eye, m, 0.0), axis=0, keepdims=True)
            o_s[r, pl.ds(258 + half, 1), :] = jnp.sum(jnp.where(eye, l, 0.0), axis=0, keepdims=True)

        @pl.when(t == 1)
        def _():
            send_a.start()

        @pl.when(t == 3)
        def _():
            send_a.wait_recv()
            for q in range(PAIR):
                merge_into(ob.at[q], o_s.at[pair["x"] + q], rba.at[q])
            send_x.start()

        @pl.when(t == 5)
        def _():
            send_b.start()

        @pl.when(t < 8 - RING)
        def _():
            for c in cache_copies(t + RING):
                c.start()

        return 0

    lax.fori_loop(0, 8, block, 0)
    send_b.wait_recv()
    for q in range(PAIR):
        merge_into(ob.at[2 + q], o_s.at[pair["own"] + q], rbb.at[q])
    send_x.wait_recv()
    for q in range(PAIR):

        def put(g, v):
            ofin[pl.ds(q * 256 + g * 128, 128), :] = v

        merge(ob.at[2 + q], rbx.at[q], put, True)
    for h in range(QH):
        obf[:, h * HD : (h + 1) * HD] = ofin[pl.ds(h, 32, stride=QH), :].astype(BF16)

    for c in ocp:
        c.wait()
    for i in range(4):
        v = jnp.concatenate(
            [
                jnp.dot(obf[...], wbuf[i, 2048 * k : 2048 * (k + 1), :], preferred_element_type=F32)
                for k in range(PAIR)
            ],
            axis=1,
        )
        cs = pl.ds(i * 1024, 1024)
        own_out[:, cs] = jnp.where(yi == 0, v[:16], v[16:])
        oth_out[:, cs] = jnp.where(yi == 0, v[16:], v[:16])
    for c in qcp + [send_a, send_b, send_x]:
        c.wait_send()


def run_front(pos, x, gain, wq, wk, wv, wo, k_blk, v_blk):
    half_idx = np.arange(HD // 2, dtype=np.float32)
    inv = (1.0 / np.power(np.float32(ROPE_THETA), np.float32(2.0) * half_idx / np.float32(HD))).astype(np.float32)
    freq = jnp.asarray(np.repeat(inv, 2)[None, :])
    vm = pl.BlockSpec(memory_space=pltpu.VMEM)
    hbm = pl.BlockSpec(memory_space=pl.ANY)
    ring = pltpu.VMEM((RING, 16, SLOTS * KVH, HD), BF16)
    dup = jax.ShapeDtypeStruct((ROWS * 8, HD), F32)
    new = jax.ShapeDtypeStruct((ROWS * KVH, HD), BF16)
    rows = jax.ShapeDtypeStruct((16, DIM), F32)
    part = pltpu.VMEM((2, 264, 128), F32)
    return pl.pallas_call(
        front_kernel,
        name="front",
        out_shape=[new, new, dup, dup, rows, rows],
        in_specs=[pl.BlockSpec(memory_space=pltpu.SMEM), vm, vm, vm, vm] + [hbm] * 6,
        out_specs=[vm] * 6,
        scratch_shapes=[
            pltpu.VMEM((ROWS, DIM), BF16),
            pltpu.VMEM((4, DIM, 512), BF16),
            ring,
            ring,
            pltpu.VMEM((QH, ROWS, HD), F32),
            pltpu.VMEM((2, KVH, ROWS, HD), F32),
            pltpu.VMEM((ROWS * QH, HD), F32),
            pltpu.VMEM((SLOTS * KVH, HD), BF16),
            pltpu.VMEM((8, 264, 128), F32),
            part,
            part,
            part,
            pltpu.VMEM((4, 264, 128), F32),
            pltpu.VMEM((512, 128), F32),
            pltpu.VMEM((32, 2048), BF16),
            pltpu.SemaphoreType.DMA((12,)),
            pltpu.SemaphoreType.DMA((2, RING)),
            pltpu.SemaphoreType.DMA((4, 2)),
            pltpu.SemaphoreType.DMA((3, 2)),
        ],
        compiler_params=pltpu.CompilerParams(
            collective_id=1, has_side_effects=True, vmem_limit_bytes=56 * MIB
        ),
        cost_estimate=pl.CostEstimate(flops=4 * 10**9, bytes_accessed=63 * 10**6, transcendentals=10**6),
    )(
        pos, x, pos[None, :], freq, gain.reshape(32, 128), wq, wk, wv, wo,
        k_blk.reshape(ROWS, SLOTS * KVH, HD), v_blk.reshape(ROWS, SLOTS * KVH, HD),
    )


def write_kernel(pos_s, kdup, vdup, kn, vn, k_in, v_in, k_out, v_out, kn_out, vn_out, tok, kbuf, vbuf, isem, osem):
    sp = lax.axis_index("sp")

    def copies_in(i, s):
        rows = pl.ds(i * WROWS, WROWS)
        return (
            pltpu.make_async_copy(k_in.at[rows], kbuf.at[s], isem.at[0, s]),
            pltpu.make_async_copy(v_in.at[rows], vbuf.at[s], isem.at[1, s]),
        )

    def copies_out(i, s):
        rows = pl.ds(i * WROWS, WROWS)
        return (
            pltpu.make_async_copy(kbuf.at[s], k_out.at[rows], osem.at[0, s]),
            pltpu.make_async_copy(vbuf.at[s], v_out.at[rows], osem.at[1, s]),
        )

    for i in range(WSTEPS):
        for c in copies_in(i, i):
            c.start()
    kn_out[...] = kn[...]
    vn_out[...] = vn[...]
    tok[...] = jnp.zeros_like(tok)
    r16 = lax.broadcasted_iota(jnp.int32, (16, HD), 0) >> 2

    def block(r, _):
        s = r
        for c in copies_in(r, s):
            c.wait()
        for b in range(WROWS):
            row = r * WROWS + b
            lim = pos_s[row] - sp * SLOTS
            cl = jnp.clip(lim, 0, SLOTS - 1)
            at = pl.ds(pl.multiple_of((cl >> 2) * 16, 16), 16)
            hit = r16 == jnp.where(lim == cl, cl & 3, -1)
            new = pl.ds(pl.multiple_of(row * 8, 8), 8)
            for dup, buf in ((kdup, kbuf), (vdup, vbuf)):
                d = dup[new, :]
                d = jnp.concatenate([d, d], axis=0).astype(BF16)
                buf[s, b, at, :] = jnp.where(hit, d, buf[s, b, at, :])
        return 0

    lax.fori_loop(0, WSTEPS, block, 0)
    for i in range(WSTEPS):
        for c in copies_out(i, i):
            c.start()
    for i in range(WSTEPS):
        for c in copies_out(i, i):
            c.wait()


def run_write(pos, kdup, vdup, kn, vn, k_blk, v_blk):
    vm = pl.BlockSpec(memory_space=pltpu.VMEM)
    hbm = pl.BlockSpec(memory_space=pl.ANY)
    cache = jax.ShapeDtypeStruct((ROWS, SLOTS * KVH, HD), BF16)
    new = jax.ShapeDtypeStruct((ROWS * KVH, HD), BF16)
    ring = pltpu.VMEM((WSTEPS, WROWS, SLOTS * KVH, HD), BF16)
    return pl.pallas_call(
        write_kernel,
        name="write",
        out_shape=[cache, cache, new, new, jax.ShapeDtypeStruct((8, 128), F32)],
        in_specs=[pl.BlockSpec(memory_space=pltpu.SMEM), vm, vm, vm, vm, hbm, hbm],
        out_specs=[hbm, hbm, vm, vm, vm],
        scratch_shapes=[
            ring,
            ring,
            pltpu.SemaphoreType.DMA((2, WSTEPS)),
            pltpu.SemaphoreType.DMA((2, WSTEPS)),
        ],
        compiler_params=pltpu.CompilerParams(vmem_limit_bytes=56 * MIB),
        cost_estimate=pl.CostEstimate(flops=5 * 10**9, bytes_accessed=67 * 10**6, transcendentals=0),
    )(
        pos, kdup, vdup, kn, vn,
        k_blk.reshape(ROWS, SLOTS * KVH, HD), v_blk.reshape(ROWS, SLOTS * KVH, HD),
    )


WROWS = 16
WSTEPS = ROWS // WROWS
NG = 4
GW = DIM // NG
TAIL_VMEM = 62 * MIB + MIB // 2
NC = 4
CW = DIM // NC
HC = CW // 2


def tail_kernel(
    own_in, oth_in, x_in, gain_ref, wg, wu, wd, tok,
    out_ref,
    wd_v, wg_v, wu_v, hs, xs, gat, nbf, act,
    part, rd, r1, r2, gat2, wsem, gsem, fsem,
):
    del tok
    sp, yi, core, xi, oc, ox, dev_c, dev_x, dev_y = place()
    oy = 1 - yi
    me, me_x, me_y, me_xy = (block_of(core, a, b) for a, b in ((xi, yi), (ox, yi), (xi, oy), (ox, oy)))

    bar = pltpu.get_barrier_semaphore()
    for dev in (dev_c, dev_x, dev_y):
        pl.semaphore_signal(bar, inc=1, device_id=dev, device_id_type=MESH)

    hcols = pl.ds(pl.multiple_of(sp * HSL, 128), HSL)
    cx = pltpu.make_async_copy(x_in.at[me], xs, wsem.at[0])
    cx.start()
    cup = []
    for j in range(NG):
        ks = pl.ds(j * GW, GW)
        cup.append(
            [
                pltpu.make_async_copy(wg.at[ks, hcols], wg_v.at[ks], wsem.at[2 + 2 * j]),
                pltpu.make_async_copy(wu.at[ks, hcols], wu_v.at[ks], wsem.at[3 + 2 * j]),
            ]
        )
        for c in cup[j]:
            c.start()
    cwd = pltpu.make_async_copy(wd.at[hcols], wd_v, wsem.at[1])
    cwd.start()
    cx.wait()
    hs[...] = xs[...].astype(F32) + (own_in[...] + oth_in[...])
    gat[me] = rms(hs[...], gain_ref).astype(BF16).astype(F32)
    pl.semaphore_wait(bar, 3)

    def gather0(buf, c0, w, sems):
        cs = pl.ds(c0, w)
        out = []
        for k, dev in ((0, dev_x), (1, dev_y), (2, dev_c)):
            c = rc(buf.at[me, :, cs], buf.at[me, :, cs], sems.at[k], dev)
            c.start()
            out.append(c)
        return out

    def gather1(buf, c0, w, sems, cps):
        lo, hi, cs = pl.ds(c0, w // 2), pl.ds(c0 + w // 2, w // 2), pl.ds(c0, w)
        cps[0].wait_recv()
        a = rc(buf.at[me_x, :, lo], buf.at[me_x, :, lo], sems.at[3], dev_y)
        a.start()
        b = rc(buf.at[me_x, :, cs], buf.at[me_x, :, cs], sems.at[4], dev_c)
        b.start()
        cps[1].wait_recv()
        c = rc(buf.at[me_y, :, hi], buf.at[me_y, :, hi], sems.at[5], dev_x)
        c.start()
        d = rc(buf.at[me_y, :, cs], buf.at[me_y, :, cs], sems.at[6], dev_c)
        d.start()
        return [a, b, c, d]

    def gather2(buf, c0, w, sems, cps):
        cs = pl.ds(c0, w)
        cps[0].wait_recv()
        cps[2].wait_recv()
        c = rc(buf.at[me_xy, :, cs], buf.at[me_xy, :, cs], sems.at[7], dev_c)
        c.start()
        return [c]

    g0 = [gather0(gat, j * GW, GW, gsem.at[j]) for j in range(NG)]
    g1 = [gather1(gat, j * GW, GW, gsem.at[j], g0[j]) for j in range(NG)]
    g2 = []

    def up(j):
        for c in (g0[j][2], g1[j][1], g1[j][3], g2[j][0]):
            c.wait_recv()
        ks = pl.ds(j * GW, GW)
        for r in range(8):
            nbf[pl.ds(r * 16, 16), :] = gat[r, :, ks].astype(BF16)

        for c in cup[j]:
            c.wait()
        for w, base in ((wg_v, 0), (wu_v, HSL)):
            v = jnp.dot(nbf[...], w[ks, :], preferred_element_type=F32).reshape(8, 16, HSL)
            cols = pl.ds(base, HSL)
            part[:, :, cols] = v if j == 0 else part[:, :, cols] + v

    for j in range(NG):
        g2.append(gather2(gat, j * GW, GW, gsem.at[j], g1[j]))
        if j:
            up(j - 1)
    up(NG - 1)

    def gate(i, _):
        cols = pl.ds(pl.multiple_of(i * 256, 256), 256)
        g = part[:, :, cols].reshape(ROWS, 256)
        u = part[:, :, pl.ds(pl.multiple_of(HSL + i * 256, 256), 256)].reshape(ROWS, 256)
        act[:, cols] = (jax.nn.silu(g) * u).astype(BF16)
        return 0

    lax.fori_loop(0, HSL // 256, gate, 0)
    cwd.wait()

    state = [dict() for _ in range(NC)]

    def s0(j):
        cs = pl.ds(j * CW, CW)
        v = jnp.dot(act[...], wd_v[:, cs], preferred_element_type=F32)
        part[:, :, cs] = v.reshape(8, 16, CW)
        c = rc(part.at[pl.ds(4 * oc, 4), :, cs], rd.at[:, :, cs], fsem.at[j, 8], dev_c)
        c.start()
        state[j]["d"] = c

    def s1(j):
        cs = pl.ds(j * CW, CW)
        state[j]["d"].wait()
        mine = pl.ds(4 * core, 4)
        rd[:, :, cs] = part[mine, :, cs] + rd[:, :, cs]
        if j % 2 == 0:
            c = [rc(rd.at[pl.ds(2 * ox, 2), :, cs], r1.at[:, :, cs], fsem.at[j, 9], dev_x)]
        else:
            c = [
                rc(rd.at[2 * i + oy, :, cs], r1.at[i, :, cs], fsem.at[j, 9 + i], dev_y)
                for i in range(PAIR)
            ]
        for k in c:
            k.start()
        state[j]["r"] = c

    def s2(j):
        cs = pl.ds(j * CW, CW)
        for k in state[j]["r"]:
            k.wait_recv()
        if j % 2 == 0:
            for i in range(PAIR):
                r1[i, :, cs] = r1[i, :, cs] + rd[2 * xi + i, :, cs]
            c = rc(r1.at[oy, :, cs], r2.at[:, cs], fsem.at[j, 11], dev_y)
        else:
            for i in range(PAIR):
                r1[i, :, cs] = r1[i, :, cs] + rd[2 * i + yi, :, cs]
            c = rc(r1.at[ox, :, cs], r2.at[:, cs], fsem.at[j, 11], dev_x)
        c.start()
        state[j]["r2"] = c

    def s3(j):
        cs = pl.ds(j * CW, CW)
        state[j]["r2"].wait_recv()
        own = r1[yi, :, cs] if j % 2 == 0 else r1[xi, :, cs]
        y = hs[:, cs] + (own + r2[:, cs])
        gat2[me, :, cs] = y.astype(BF16).astype(F32)
        state[j]["g0"] = gather0(gat2, j * CW, CW, fsem.at[j])

    def s4(j):
        state[j]["g1"] = gather1(gat2, j * CW, CW, fsem.at[j], state[j]["g0"])

    def s5(j):
        state[j]["g2"] = gather2(gat2, j * CW, CW, fsem.at[j], state[j]["g1"])

    def s6(j):
        cs = pl.ds(j * CW, CW)
        st = state[j]
        for c in (st["g0"][2], st["g1"][1], st["g1"][3], st["g2"][0]):
            c.wait_recv()
        out_ref[:, :, cs] = gat2[:, :, cs].astype(BF16)

    for t in range(NC + 1):
        if t < NC:
            s0(t)
        if t:
            s1(t - 1)
    for stage in (s2, s3, s4, s5, s6):
        for j in range(NC):
            stage(j)

    for c in sum(g0 + g1 + g2, []):
        c.wait_send()
    for st in state:
        for c in st["r"] + [st["r2"]] + st["g0"] + st["g1"] + st["g2"]:
            c.wait_send()


def run_tail(own, oth, x, gain, wg, wu, wd, tok):
    vm = pl.BlockSpec(memory_space=pltpu.VMEM)
    hbm = pl.BlockSpec(memory_space=pl.ANY)
    return pl.pallas_call(
        tail_kernel,
        name="tail",
        out_shape=pltpu.VMEM((8, 16, DIM), BF16),
        in_specs=[vm, vm, hbm, vm, hbm, hbm, hbm, hbm],
        out_specs=vm,
        scratch_shapes=[
            pltpu.VMEM((HSL, DIM), BF16),
            pltpu.VMEM((DIM, HSL), BF16),
            pltpu.VMEM((DIM, HSL), BF16),
            pltpu.VMEM((16, DIM), F32),
            pltpu.VMEM((16, DIM), BF16),
            pltpu.VMEM((8, 16, DIM), F32),
            pltpu.VMEM((ROWS, GW), BF16),
            pltpu.VMEM((ROWS, HSL), BF16),
            pltpu.VMEM((8, 16, DIM), F32),
            pltpu.VMEM((4, 16, DIM), F32),
            pltpu.VMEM((2, 16, DIM), F32),
            pltpu.VMEM((16, DIM), F32),
            pltpu.VMEM((8, 16, DIM), F32),
            pltpu.SemaphoreType.DMA((2 + 2 * NG,)),
            pltpu.SemaphoreType.DMA((NG, 8, 2)),
            pltpu.SemaphoreType.DMA((NC, 12, 2)),
        ],
        compiler_params=pltpu.CompilerParams(
            collective_id=0, has_side_effects=True, vmem_limit_bytes=TAIL_VMEM
        ),
        cost_estimate=pl.CostEstimate(flops=6 * 10**9, bytes_accessed=62 * 10**6, transcendentals=10**6),
    )(own, oth, x.reshape(8, 16, DIM), gain.reshape(32, 128), wg, wu, wd, tok)


def solution(mesh):
    def local_step(layer_in, new_pos, k_blk, v_blk, attn_gain, w_query, w_key, w_value, w_out, mlp_gain, w_gate, w_up, w_down):
        kn, vn, kdup, vdup, own, oth = run_front(
            new_pos, layer_in, attn_gain, w_query, w_key, w_value, w_out, k_blk, v_blk
        )
        oth = lax.ppermute(oth, 'tp', [(0, 1), (1, 0)])
        k_upd, v_upd, k_new, v_new, tok = run_write(new_pos, kdup, vdup, kn, vn, k_blk, v_blk)
        y = run_tail(own, oth, layer_in, mlp_gain, w_gate, w_up, w_down, tok)
        shape = (ROWS, SLOTS, KVH, HD)
        new = (ROWS, KVH, HD)
        return y.reshape(ROWS, DIM), k_upd.reshape(shape), v_upd.reshape(shape), k_new.reshape(new), v_new.reshape(new)

    cache_spec = P('dp', 'sp', 'tp', None)
    new_spec = P('dp', 'tp', None)
    in_specs = (P('dp', None), P('dp'), cache_spec, cache_spec, P(None), P(None, 'tp'), P(None, 'tp'), P(None, 'tp'), P('tp', None), P(None), P(None, 'tp'), P(None, 'tp'), P('tp', None))
    out_specs = (P('dp', None), cache_spec, cache_spec, new_spec, new_spec)
    return jax.shard_map(local_step, mesh=mesh, in_specs=in_specs, out_specs=out_specs, check_vma=False)
```

```python
import functools

import jax
import jax.numpy as jnp
import numpy as np
from jax import lax
from jax.experimental import pallas as pl
from jax.experimental.pallas import tpu as pltpu
from jax.sharding import PartitionSpec as P

ROPE_THETA = 1000000
MESH = pl.DeviceIdType.MESH
F32 = jnp.float32
BF16 = jnp.bfloat16
MIB = 2**20
VMEM_MAX = 67043328

ROWS = 128
DIM = 4096
HD = 128
SLOTS = 128
KVH = 4
QH = 16
HID = 7168
HSL = HID // 4
NEG = -1e30
PAIR = 2
M_AT = pl.ds(256, PAIR)
L_AT = pl.ds(258, PAIR)
RING = 6

def rms(x, gain_ref):
    ms = jnp.mean(jnp.square(x), axis=-1, keepdims=True)
    gain = gain_ref[...].astype(F32)
    gain = jnp.concatenate([gain[j : j + 1, :] for j in range(DIM // 128)], axis=1)
    return x * lax.rsqrt(ms + 1e-5) * gain


def column(v):
    return jnp.transpose(jnp.broadcast_to(v, (128, 128)))


def place():
    sp = lax.axis_index("sp")
    yi = lax.axis_index("tp")
    dp = lax.axis_index("dp")
    core = lax.rem(sp, 2)
    xi = sp // 2
    oc = 1 - core
    ox = 1 - xi
    return sp, yi, core, xi, oc, ox, (dp, yi, 2 * xi + oc), (dp, yi, 2 * ox + core), (dp, 1 - yi, sp)


def block_of(c, x, y):
    return 4 * c + 2 * x + y


def rc(src, dst, sems, dev):
    return pltpu.make_async_remote_copy(
        src_ref=src, dst_ref=dst, send_sem=sems.at[0], recv_sem=sems.at[1],
        device_id=dev, device_id_type=MESH,
    )


def front_kernel(
    pos_s, x_ref, pos_v, freq_ref, gain_ref, wq, wk, wv, wo, k_in, v_in,
    kn_out, vn_out, kdup, vdup, own_out, oth_out,
    n_s, wbuf, kbuf, vbuf, qraw, kvraw, qf, slotb, o_s, rba, rbb, rbx, ob, ofin, obf,
    wsem, isem, qsem, bsem,
):
    sp, yi, core, xi, oc, ox, dev_c, dev_x, dev_y = place()

    bar = pltpu.get_barrier_semaphore()
    for dev in (dev_c, dev_x):
        pl.semaphore_signal(bar, inc=1, device_id=dev, device_id_type=MESH)

    def row_block(t):
        p, y = t // 2, t % 2
        c = core + (oc - core) * (1 - p % 2)
        x = xi + (ox - xi) * (1 - p // 2)
        return block_of(c, x, y)

    def cache_copies(t):
        rows = pl.ds(row_block(t) * 16, 16)
        return (
            pltpu.make_async_copy(k_in.at[rows], kbuf.at[t % RING], isem.at[0, t % RING]),
            pltpu.make_async_copy(v_in.at[rows], vbuf.at[t % RING], isem.at[1, t % RING]),
        )

    def cols(start, width):
        return pl.ds(pl.multiple_of(start, 128), width)

    wcp = [
        [
            pltpu.make_async_copy(wk.at[:, cols(core * 256, 256)], wbuf.at[0, :, pl.ds(0, 256)], wsem.at[0]),
            pltpu.make_async_copy(wv.at[:, cols(core * 256, 256)], wbuf.at[0, :, pl.ds(256, 256)], wsem.at[1]),
        ],
        [pltpu.make_async_copy(wq.at[:, cols(core * 1024, 512)], wbuf.at[1], wsem.at[2])],
        [pltpu.make_async_copy(wq.at[:, cols(core * 1024 + 512, 512)], wbuf.at[2], wsem.at[3])],
    ]
    ocp = [
        pltpu.make_async_copy(
            wo.at[:, pl.ds(512 * i, 512)], wbuf.at[i // 2, pl.ds(2048 * (i % 2), 2048)], wsem.at[4 + i]
        )
        for i in range(8)
    ]
    for group in wcp:
        for c in group:
            c.start()
    for c in cache_copies(0):
        c.start()

    n_s[...] = rms(x_ref[...].astype(F32), gain_ref).astype(BF16)
    ang = column(pos_v[...].astype(F32)) * freq_ref[...]
    lane = lax.broadcasted_iota(jnp.int32, (ROWS, HD), 1)
    even = (lane & 1) == 0
    cosr = jnp.cos(ang)
    sinr = jnp.sin(ang)
    sinr = jnp.where(even, -sinr, sinr)
    slotb[...] = (lax.broadcasted_iota(jnp.int32, (SLOTS * KVH, HD), 0) >> 2).astype(F32).astype(BF16)

    def rotate(y):
        swap = jnp.where(even, pltpu.roll(y, HD - 1, 1), pltpu.roll(y, 1, 1))
        return y * cosr + swap * sinr

    qcp = []
    for j in range(3):
        for c in wcp[j]:
            c.wait()
        y = jnp.dot(n_s[...], wbuf[j], preferred_element_type=F32)
        for t in range(1 + j, RING if j == 2 else 2 + j):
            for c in cache_copies(t):
                c.start()
        for hh in range(4):
            yh = y[:, hh * HD : (hh + 1) * HD]
            if j == 0 and hh < 2:
                kvraw[0, 2 * core + hh] = rotate(yh)
            elif j == 0:
                kvraw[1, 2 * core + hh - 2] = yh
            else:
                qraw[8 * core + (j - 1) * 4 + hh] = rotate(yh)
        if j == 0:
            pl.semaphore_wait(bar, 2)
            for i in range(PAIR):
                ref = kvraw.at[i, pl.ds(2 * core, 2)]
                qcp.append(rc(ref, ref, qsem.at[i], dev_c))
        else:
            ref = qraw.at[pl.ds(8 * core + (j - 1) * 4, 4)]
            qcp.append(rc(ref, ref, qsem.at[1 + j], dev_c))
            if j == 1:
                qcp[0].start()
                qcp[1].start()
                qcp[2].start()
            else:
                qcp[3].start()
    for c in qcp:
        c.wait_recv()
    for i, (dup, out) in enumerate(((kdup, kn_out), (vdup, vn_out))):
        for h in range(KVH):
            v = kvraw[i, h]
            ofin[pl.ds(h, ROWS, stride=KVH), :] = v
            for rep in range(PAIR):
                dup[pl.ds(rep * KVH + h, ROWS, stride=8), :] = v
        out[...] = ofin[...].astype(BF16)
    for h in range(QH):
        qf[pl.ds(h, ROWS, stride=QH), :] = qraw[h]

    col = lax.broadcasted_iota(jnp.int32, (QH, SLOTS * KVH), 1)
    hrow = lax.broadcasted_iota(jnp.int32, (QH, SLOTS * KVH), 0)
    slot_id = jnp.where((col & 3) == (hrow >> 2), col >> 2, jnp.int32(1 << 20))
    eye = lax.broadcasted_iota(jnp.int32, (128, 128), 0) == lax.broadcasted_iota(
        jnp.int32, (128, 128), 1
    )

    def merge(a, b, put, last):
        m1, m2 = a[M_AT, :], b[M_AT, :]
        l1, l2 = a[L_AT, :], b[L_AT, :]
        m = jnp.maximum(m1, m2)
        a1 = jnp.exp(m1 - m)
        a2 = jnp.exp(m2 - m)
        l = a1 * l1 + a2 * l2
        if last:
            a1 = a1 / l
            a2 = a2 / l
        for g in range(PAIR):
            rows = pl.ds(g * 128, 128)
            put(g, column(a1[g : g + 1]) * a[rows, :] + column(a2[g : g + 1]) * b[rows, :])
        return m, l

    def merge_into(dst, a, b):
        def put(g, v):
            dst[pl.ds(g * 128, 128), :] = v

        m, l = merge(a, b, put, False)
        dst[M_AT, :] = m
        dst[L_AT, :] = l

    pair = {
        "a": block_of(oc, ox, 0),
        "x": block_of(core, ox, 0),
        "b": block_of(oc, xi, 0),
        "own": block_of(core, xi, 0),
    }
    send_a = rc(o_s.at[pl.ds(pair["a"], 2)], rba, bsem.at[0], dev_c)
    send_b = rc(o_s.at[pl.ds(pair["b"], 2)], rbb, bsem.at[1], dev_c)
    send_x = [rc(ob.at[q], rbx.at[q], bsem.at[2 + q], dev_x) for q in range(PAIR)]

    def patched(dup, buf, t, b, row, lim):
        hit = slotb[...] == lax.broadcast(lim.astype(F32), (SLOTS * KVH, HD)).astype(BF16)
        d = dup[pl.ds(pl.multiple_of(row * 8, 8), 8), :]
        d = jnp.concatenate([d, d], axis=0).astype(BF16)
        d = jnp.concatenate([d] * 32, axis=0)
        return jnp.where(hit, d, buf[t % RING, b])

    def block(t, _):
        r = row_block(t)
        for c in cache_copies(t):
            c.wait()

        @pl.when(t == 2)
        def _():
            for c in ocp:
                c.start()

        for half in range(PAIR):
            sc, lims = [], []
            for b in range(8):
                row = r * 16 + half * 8 + b
                lim = pos_s[row] - sp * SLOTS
                lims.append(lim)
                q = qf[pl.ds(pl.multiple_of(row * QH, QH), QH), :].astype(BF16)
                sc.append(
                    lax.dot_general(
                        q, patched(kdup, kbuf, t, half * 8 + b, row, lim), (((1,), (1,)), ((), ())), preferred_element_type=F32
                    )
                )
            ms, ls = [], []
            for b in range(8):
                ok = slot_id <= lims[b]
                s = jnp.where(ok, sc[b] * (HD**-0.5), NEG)
                m = jnp.maximum(jnp.max(s, axis=-1, keepdims=True), NEG * 0.1)
                w = jnp.exp(s - m)
                ms.append(m)
                ls.append(jnp.sum(w, axis=-1, keepdims=True))
                v = patched(vdup, vbuf, t, half * 8 + b, r * 16 + half * 8 + b, lims[b])
                o = jnp.dot(w.astype(BF16), v, preferred_element_type=F32)
                o_s[r, pl.ds((half * 8 + b) * QH, QH), :] = o
            m = jnp.concatenate(ms, axis=0)
            l = jnp.concatenate(ls, axis=0)
            o_s[r, pl.ds(256 + half, 1), :] = jnp.sum(jnp.where(eye, m, 0.0), axis=0, keepdims=True)
            o_s[r, pl.ds(258 + half, 1), :] = jnp.sum(jnp.where(eye, l, 0.0), axis=0, keepdims=True)

        @pl.when(t == 1)
        def _():
            send_a.start()

        for q in range(PAIR):

            @pl.when(t == 2 + q)
            def _():
                if q == 0:
                    send_a.wait_recv()
                merge_into(ob.at[q], o_s.at[pair["x"] + q], rba.at[q])
                send_x[q].start()

        @pl.when(t == 5)
        def _():
            send_b.start()

        @pl.when(t < 8 - RING)
        def _():
            for c in cache_copies(t + RING):
                c.start()

        return 0

    lax.fori_loop(0, 8, block, 0)
    send_b.wait_recv()
    for q in range(PAIR):
        merge_into(ob.at[2 + q], o_s.at[pair["own"] + q], rbb.at[q])
    for q in range(PAIR):
        send_x[q].wait_recv()

        def put(g, v):
            ofin[pl.ds(q * 256 + g * 128, 128), :] = v

        merge(ob.at[2 + q], rbx.at[q], put, True)
    for h in range(QH):
        obf[:, h * HD : (h + 1) * HD] = ofin[pl.ds(h, 32, stride=QH), :].astype(BF16)

    for c in ocp:
        c.wait()
    for i in range(4):
        v = jnp.concatenate(
            [
                jnp.dot(obf[...], wbuf[i, 2048 * k : 2048 * (k + 1), :], preferred_element_type=F32)
                for k in range(PAIR)
            ],
            axis=1,
        )
        cs = pl.ds(i * 1024, 1024)
        own_out[:, cs] = jnp.where(yi == 0, v[:16], v[16:])
        oth_out[:, cs] = jnp.where(yi == 0, v[16:], v[:16])
    for c in qcp + send_x + [send_a, send_b]:
        c.wait_send()


def run_front(pos, x, gain, wq, wk, wv, wo, k_blk, v_blk):
    half_idx = np.arange(HD // 2, dtype=np.float32)
    inv = (1.0 / np.power(np.float32(ROPE_THETA), np.float32(2.0) * half_idx / np.float32(HD))).astype(np.float32)
    freq = jnp.asarray(np.repeat(inv, 2)[None, :])
    vm = pl.BlockSpec(memory_space=pltpu.VMEM)
    hbm = pl.BlockSpec(memory_space=pl.ANY)
    ring = pltpu.VMEM((RING, 16, SLOTS * KVH, HD), BF16)
    dup = jax.ShapeDtypeStruct((ROWS * 8, HD), F32)
    new = jax.ShapeDtypeStruct((ROWS * KVH, HD), BF16)
    rows = jax.ShapeDtypeStruct((16, DIM), F32)
    part = pltpu.VMEM((2, 264, 128), F32)
    return pl.pallas_call(
        front_kernel,
        name="front",
        out_shape=[new, new, dup, dup, rows, rows],
        in_specs=[pl.BlockSpec(memory_space=pltpu.SMEM), vm, vm, vm, vm] + [hbm] * 6,
        out_specs=[vm] * 6,
        scratch_shapes=[
            pltpu.VMEM((ROWS, DIM), BF16),
            pltpu.VMEM((4, DIM, 512), BF16),
            ring,
            ring,
            pltpu.VMEM((QH, ROWS, HD), F32),
            pltpu.VMEM((2, KVH, ROWS, HD), F32),
            pltpu.VMEM((ROWS * QH, HD), F32),
            pltpu.VMEM((SLOTS * KVH, HD), BF16),
            pltpu.VMEM((8, 264, 128), F32),
            part,
            part,
            part,
            pltpu.VMEM((4, 264, 128), F32),
            pltpu.VMEM((512, 128), F32),
            pltpu.VMEM((32, 2048), BF16),
            pltpu.SemaphoreType.DMA((12,)),
            pltpu.SemaphoreType.DMA((2, RING)),
            pltpu.SemaphoreType.DMA((4, 2)),
            pltpu.SemaphoreType.DMA((4, 2)),
        ],
        compiler_params=pltpu.CompilerParams(
            collective_id=1, has_side_effects=True, vmem_limit_bytes=60 * MIB
        ),
        cost_estimate=pl.CostEstimate(flops=4 * 10**9, bytes_accessed=63 * 10**6, transcendentals=10**6),
    )(
        pos, x, pos[None, :], freq, gain.reshape(32, 128), wq, wk, wv, wo,
        k_blk.reshape(ROWS, SLOTS * KVH, HD), v_blk.reshape(ROWS, SLOTS * KVH, HD),
    )


def write_kernel(
    pos_s, kdup_in, vdup_in, kn_in, vn_in, k_in, v_in,
    k_out, v_out, kn_out, vn_out, tok,
    kbuf, vbuf, kdup, vdup, kn, vn, isem, osem, ssem, nsem,
):
    sp = lax.axis_index("sp")

    def copies_in(i, s):
        rows = pl.ds(i * WROWS, WROWS)
        return (
            pltpu.make_async_copy(k_in.at[rows], kbuf.at[s], isem.at[0, s]),
            pltpu.make_async_copy(v_in.at[rows], vbuf.at[s], isem.at[1, s]),
        )

    def copies_out(i, s):
        rows = pl.ds(i * WROWS, WROWS)
        return (
            pltpu.make_async_copy(kbuf.at[s], k_out.at[rows], osem.at[0, s]),
            pltpu.make_async_copy(vbuf.at[s], v_out.at[rows], osem.at[1, s]),
        )

    small = [
        pltpu.make_async_copy(a, b, ssem.at[i])
        for i, (a, b) in enumerate(((kdup_in, kdup), (vdup_in, vdup), (kn_in, kn), (vn_in, vn)))
    ]
    new = [
        pltpu.make_async_copy(a, b, nsem.at[i]) for i, (a, b) in enumerate(((kn, kn_out), (vn, vn_out)))
    ]
    for c in small:
        c.start()
    for i in range(WSTEPS):
        for c in copies_in(i, i):
            c.start()
    tok[...] = jnp.zeros_like(tok)
    for c in small:
        c.wait()
    for c in new:
        c.start()
    r16 = lax.broadcasted_iota(jnp.int32, (16, HD), 0) >> 2

    def block(r, _):
        s = r
        for c in copies_in(r, s):
            c.wait()
        for b in range(WROWS):
            row = r * WROWS + b
            lim = pos_s[row] - sp * SLOTS
            cl = jnp.clip(lim, 0, SLOTS - 1)
            at = pl.ds(pl.multiple_of((cl >> 2) * 16, 16), 16)
            hit = r16 == jnp.where(lim == cl, cl & 3, -1)
            of_row = pl.ds(pl.multiple_of(row * 8, 8), 8)
            for dup, buf in ((kdup, kbuf), (vdup, vbuf)):
                d = dup[of_row, :]
                d = jnp.concatenate([d, d], axis=0).astype(BF16)
                buf[s, b, at, :] = jnp.where(hit, d, buf[s, b, at, :])
        return 0

    lax.fori_loop(0, WSTEPS, block, 0)
    for i in range(WSTEPS):
        for c in copies_out(i, i):
            c.start()
    for i in range(WSTEPS):
        for c in copies_out(i, i):
            c.wait()
    for c in new:
        c.wait()


def run_write(pos, kdup, vdup, kn, vn, k_blk, v_blk):
    vm = pl.BlockSpec(memory_space=pltpu.VMEM)
    hbm = pl.BlockSpec(memory_space=pl.ANY)
    cache = jax.ShapeDtypeStruct((ROWS, SLOTS * KVH, HD), BF16)
    new = jax.ShapeDtypeStruct((ROWS * KVH, HD), BF16)
    dup = pltpu.VMEM((ROWS * 8, HD), F32)
    small = pltpu.VMEM((ROWS * KVH, HD), BF16)
    ring = pltpu.VMEM((WSTEPS, WROWS, SLOTS * KVH, HD), BF16)
    return pl.pallas_call(
        write_kernel,
        name="write",
        out_shape=[cache, cache, new, new, jax.ShapeDtypeStruct((8, 128), F32)],
        in_specs=[pl.BlockSpec(memory_space=pltpu.SMEM)] + [hbm] * 6,
        out_specs=[hbm] * 4 + [vm],
        scratch_shapes=[
            ring,
            ring,
            dup,
            dup,
            small,
            small,
            pltpu.SemaphoreType.DMA((2, WSTEPS)),
            pltpu.SemaphoreType.DMA((2, WSTEPS)),
            pltpu.SemaphoreType.DMA((4,)),
            pltpu.SemaphoreType.DMA((2,)),
        ],
        compiler_params=pltpu.CompilerParams(vmem_limit_bytes=VMEM_MAX),
        cost_estimate=pl.CostEstimate(flops=5 * 10**9, bytes_accessed=67 * 10**6, transcendentals=0),
    )(
        pos, kdup, vdup, kn, vn,
        k_blk.reshape(ROWS, SLOTS * KVH, HD), v_blk.reshape(ROWS, SLOTS * KVH, HD),
    )


WROWS = 16
WSTEPS = ROWS // WROWS
NG = 4
GW = DIM // NG
TAIL_VMEM = 62 * MIB + MIB // 2
NC = 4
CW = DIM // NC
HC = CW // 2


def tail_kernel(
    own_in, oth_in, x_in, gain_ref, wg, wu, wd, tok,
    out_ref,
    wd_v, wg_v, wu_v, hs, xs, gat, nbf, act,
    part, rd, r1, r2, gat2, wsem, gsem, fsem,
):
    del tok
    sp, yi, core, xi, oc, ox, dev_c, dev_x, dev_y = place()
    oy = 1 - yi
    me, me_x, me_y, me_xy = (block_of(core, a, b) for a, b in ((xi, yi), (ox, yi), (xi, oy), (ox, oy)))

    bar = pltpu.get_barrier_semaphore()
    for dev in (dev_c, dev_x, dev_y):
        pl.semaphore_signal(bar, inc=1, device_id=dev, device_id_type=MESH)

    hcols = pl.ds(pl.multiple_of(sp * HSL, 128), HSL)
    cx = pltpu.make_async_copy(x_in.at[me], xs, wsem.at[0])
    cx.start()
    cup = []
    for j in range(NG):
        ks = pl.ds(j * GW, GW)
        cup.append(
            [
                pltpu.make_async_copy(wg.at[ks, hcols], wg_v.at[ks], wsem.at[2 + 2 * j]),
                pltpu.make_async_copy(wu.at[ks, hcols], wu_v.at[ks], wsem.at[3 + 2 * j]),
            ]
        )
        for c in cup[j]:
            c.start()
    cwd = pltpu.make_async_copy(wd.at[hcols], wd_v, wsem.at[1])
    cwd.start()
    cx.wait()
    hs[...] = xs[...].astype(F32) + (own_in[...] + oth_in[...])
    gat[me] = rms(hs[...], gain_ref).astype(BF16).astype(F32)
    pl.semaphore_wait(bar, 3)

    def gather0(buf, c0, w, sems):
        cs = pl.ds(c0, w)
        out = []
        for k, dev in ((0, dev_x), (1, dev_y), (2, dev_c)):
            c = rc(buf.at[me, :, cs], buf.at[me, :, cs], sems.at[k], dev)
            c.start()
            out.append(c)
        return out

    def gather1(buf, c0, w, sems, cps):
        lo, hi, cs = pl.ds(c0, w // 2), pl.ds(c0 + w // 2, w // 2), pl.ds(c0, w)
        cps[0].wait_recv()
        a = rc(buf.at[me_x, :, lo], buf.at[me_x, :, lo], sems.at[3], dev_y)
        a.start()
        b = rc(buf.at[me_x, :, cs], buf.at[me_x, :, cs], sems.at[4], dev_c)
        b.start()
        cps[1].wait_recv()
        c = rc(buf.at[me_y, :, hi], buf.at[me_y, :, hi], sems.at[5], dev_x)
        c.start()
        d = rc(buf.at[me_y, :, cs], buf.at[me_y, :, cs], sems.at[6], dev_c)
        d.start()
        return [a, b, c, d]

    def gather2(buf, c0, w, sems, cps):
        cs = pl.ds(c0, w)
        cps[0].wait_recv()
        cps[2].wait_recv()
        c = rc(buf.at[me_xy, :, cs], buf.at[me_xy, :, cs], sems.at[7], dev_c)
        c.start()
        return [c]

    g0 = [gather0(gat, j * GW, GW, gsem.at[j]) for j in range(NG)]
    g1 = [gather1(gat, j * GW, GW, gsem.at[j], g0[j]) for j in range(NG)]
    g2 = []

    def up(j):
        for c in (g0[j][2], g1[j][1], g1[j][3], g2[j][0]):
            c.wait_recv()
        ks = pl.ds(j * GW, GW)
        for r in range(8):
            nbf[pl.ds(r * 16, 16), :] = gat[r, :, ks].astype(BF16)

        for c in cup[j]:
            c.wait()
        for w, base in ((wg_v, 0), (wu_v, HSL)):
            v = jnp.dot(nbf[...], w[ks, :], preferred_element_type=F32).reshape(8, 16, HSL)
            cols = pl.ds(base, HSL)
            part[:, :, cols] = v if j == 0 else part[:, :, cols] + v

    for j in range(NG):
        g2.append(gather2(gat, j * GW, GW, gsem.at[j], g1[j]))
        if j:
            up(j - 1)
    up(NG - 1)

    def gate(i, _):
        cols = pl.ds(pl.multiple_of(i * 256, 256), 256)
        g = part[:, :, cols].reshape(ROWS, 256)
        u = part[:, :, pl.ds(pl.multiple_of(HSL + i * 256, 256), 256)].reshape(ROWS, 256)
        act[:, cols] = (jax.nn.silu(g) * u).astype(BF16)
        return 0

    lax.fori_loop(0, HSL // 256, gate, 0)
    cwd.wait()

    state = [dict() for _ in range(NC)]

    def s0(j):
        cs = pl.ds(j * CW, CW)
        v = jnp.dot(act[...], wd_v[:, cs], preferred_element_type=F32)
        part[:, :, cs] = v.reshape(8, 16, CW)
        c = rc(part.at[pl.ds(4 * oc, 4), :, cs], rd.at[:, :, cs], fsem.at[j, 8], dev_c)
        c.start()
        state[j]["d"] = c

    def s1(j):
        cs = pl.ds(j * CW, CW)
        state[j]["d"].wait()
        mine = pl.ds(4 * core, 4)
        rd[:, :, cs] = part[mine, :, cs] + rd[:, :, cs]
        if j % 2 == 0:
            c = [rc(rd.at[pl.ds(2 * ox, 2), :, cs], r1.at[:, :, cs], fsem.at[j, 9], dev_x)]
        else:
            c = [
                rc(rd.at[2 * i + oy, :, cs], r1.at[i, :, cs], fsem.at[j, 9 + i], dev_y)
                for i in range(PAIR)
            ]
        for k in c:
            k.start()
        state[j]["r"] = c

    def s2(j):
        cs = pl.ds(j * CW, CW)
        for k in state[j]["r"]:
            k.wait_recv()
        if j % 2 == 0:
            for i in range(PAIR):
                r1[i, :, cs] = r1[i, :, cs] + rd[2 * xi + i, :, cs]
            c = rc(r1.at[oy, :, cs], r2.at[:, cs], fsem.at[j, 11], dev_y)
        else:
            for i in range(PAIR):
                r1[i, :, cs] = r1[i, :, cs] + rd[2 * i + yi, :, cs]
            c = rc(r1.at[ox, :, cs], r2.at[:, cs], fsem.at[j, 11], dev_x)
        c.start()
        state[j]["r2"] = c

    def s3(j):
        cs = pl.ds(j * CW, CW)
        state[j]["r2"].wait_recv()
        own = r1[yi, :, cs] if j % 2 == 0 else r1[xi, :, cs]
        y = hs[:, cs] + (own + r2[:, cs])
        gat2[me, :, cs] = y.astype(BF16).astype(F32)
        state[j]["g0"] = gather0(gat2, j * CW, CW, fsem.at[j])

    def s4(j):
        state[j]["g1"] = gather1(gat2, j * CW, CW, fsem.at[j], state[j]["g0"])

    def s5(j):
        state[j]["g2"] = gather2(gat2, j * CW, CW, fsem.at[j], state[j]["g1"])

    def s6(j):
        cs = pl.ds(j * CW, CW)
        st = state[j]
        for c in (st["g0"][2], st["g1"][1], st["g1"][3], st["g2"][0]):
            c.wait_recv()
        out_ref[:, :, cs] = gat2[:, :, cs].astype(BF16)

    for t in range(NC + 1):
        if t < NC:
            s0(t)
        if t:
            s1(t - 1)
    for stage in (s2, s3, s4, s5, s6):
        for j in range(NC):
            stage(j)

    for c in sum(g0 + g1 + g2, []):
        c.wait_send()
    for st in state:
        for c in st["r"] + [st["r2"]] + st["g0"] + st["g1"] + st["g2"]:
            c.wait_send()


def run_tail(own, oth, x, gain, wg, wu, wd, tok):
    vm = pl.BlockSpec(memory_space=pltpu.VMEM)
    hbm = pl.BlockSpec(memory_space=pl.ANY)
    return pl.pallas_call(
        tail_kernel,
        name="tail",
        out_shape=pltpu.VMEM((8, 16, DIM), BF16),
        in_specs=[vm, vm, hbm, vm, hbm, hbm, hbm, hbm],
        out_specs=vm,
        scratch_shapes=[
            pltpu.VMEM((HSL, DIM), BF16),
            pltpu.VMEM((DIM, HSL), BF16),
            pltpu.VMEM((DIM, HSL), BF16),
            pltpu.VMEM((16, DIM), F32),
            pltpu.VMEM((16, DIM), BF16),
            pltpu.VMEM((8, 16, DIM), F32),
            pltpu.VMEM((ROWS, GW), BF16),
            pltpu.VMEM((ROWS, HSL), BF16),
            pltpu.VMEM((8, 16, DIM), F32),
            pltpu.VMEM((4, 16, DIM), F32),
            pltpu.VMEM((2, 16, DIM), F32),
            pltpu.VMEM((16, DIM), F32),
            pltpu.VMEM((8, 16, DIM), F32),
            pltpu.SemaphoreType.DMA((2 + 2 * NG,)),
            pltpu.SemaphoreType.DMA((NG, 8, 2)),
            pltpu.SemaphoreType.DMA((NC, 12, 2)),
        ],
        compiler_params=pltpu.CompilerParams(
            collective_id=0, has_side_effects=True, vmem_limit_bytes=TAIL_VMEM
        ),
        cost_estimate=pl.CostEstimate(flops=6 * 10**9, bytes_accessed=62 * 10**6, transcendentals=10**6),
    )(own, oth, x.reshape(8, 16, DIM), gain.reshape(32, 128), wg, wu, wd, tok)


def solution(mesh):
    def local_step(layer_in, new_pos, k_blk, v_blk, attn_gain, w_query, w_key, w_value, w_out, mlp_gain, w_gate, w_up, w_down):
        kn, vn, kdup, vdup, own, oth = run_front(
            new_pos, layer_in, attn_gain, w_query, w_key, w_value, w_out, k_blk, v_blk
        )
        oth = lax.ppermute(oth, 'tp', [(0, 1), (1, 0)])
        k_upd, v_upd, k_new, v_new, tok = run_write(new_pos, kdup, vdup, kn, vn, k_blk, v_blk)
        y = run_tail(own, oth, layer_in, mlp_gain, w_gate, w_up, w_down, tok)
        shape = (ROWS, SLOTS, KVH, HD)
        new = (ROWS, KVH, HD)
        return y.reshape(ROWS, DIM), k_upd.reshape(shape), v_upd.reshape(shape), k_new.reshape(new), v_new.reshape(new)

    cache_spec = P('dp', 'sp', 'tp', None)
    new_spec = P('dp', 'tp', None)
    in_specs = (P('dp', None), P('dp'), cache_spec, cache_spec, P(None), P(None, 'tp'), P(None, 'tp'), P(None, 'tp'), P('tp', None), P(None), P(None, 'tp'), P(None, 'tp'), P('tp', None))
    out_specs = (P('dp', None), cache_spec, cache_spec, new_spec, new_spec)
    return jax.shard_map(local_step, mesh=mesh, in_specs=in_specs, out_specs=out_specs, check_vma=False)
```

```python
import functools

import jax
import jax.numpy as jnp
import numpy as np
from jax import lax
from jax.experimental import pallas as pl
from jax.experimental.pallas import tpu as pltpu
from jax.sharding import PartitionSpec as P

ROPE_THETA = 1000000
MESH = pl.DeviceIdType.MESH
F32 = jnp.float32
BF16 = jnp.bfloat16
MIB = 2**20
VMEM_MAX = 67043328

ROWS = 128
DIM = 4096
HD = 128
SLOTS = 128
KVH = 4
QH = 16
HID = 7168
HSL = HID // 4
NEG = -1e30
PAIR = 2
M_AT = pl.ds(256, PAIR)
L_AT = pl.ds(258, PAIR)
RING = 6

def rms(x, gain_ref):
    ms = jnp.mean(jnp.square(x), axis=-1, keepdims=True)
    gain = gain_ref[...].astype(F32)
    gain = jnp.concatenate([gain[j : j + 1, :] for j in range(DIM // 128)], axis=1)
    return x * lax.rsqrt(ms + 1e-5) * gain


def column(v):
    return jnp.transpose(jnp.broadcast_to(v, (128, 128)))


def place():
    sp = lax.axis_index("sp")
    yi = lax.axis_index("tp")
    dp = lax.axis_index("dp")
    core = lax.rem(sp, 2)
    xi = sp // 2
    oc = 1 - core
    ox = 1 - xi
    return sp, yi, core, xi, oc, ox, (dp, yi, 2 * xi + oc), (dp, yi, 2 * ox + core), (dp, 1 - yi, sp)


def block_of(c, x, y):
    return 4 * c + 2 * x + y


def rc(src, dst, sems, dev):
    return pltpu.make_async_remote_copy(
        src_ref=src, dst_ref=dst, send_sem=sems.at[0], recv_sem=sems.at[1],
        device_id=dev, device_id_type=MESH,
    )


def front_kernel(
    pos_s, x_ref, pos_v, freq_ref, gain_ref, wq, wk, wv, wo, k_in, v_in,
    kn_out, vn_out, kdup, vdup, own_out, oth_out,
    n_s, wbuf, kbuf, vbuf, qraw, kvraw, qf, slotb, o_s, rba, rbb, rbx, ob, ofin, obf,
    wsem, isem, qsem, bsem,
):
    sp, yi, core, xi, oc, ox, dev_c, dev_x, dev_y = place()

    bar = pltpu.get_barrier_semaphore()
    for dev in (dev_c, dev_x):
        pl.semaphore_signal(bar, inc=1, device_id=dev, device_id_type=MESH)

    def row_block(t):
        p, y = t // 2, t % 2
        c = core + (oc - core) * (1 - p % 2)
        x = xi + (ox - xi) * (1 - p // 2)
        return block_of(c, x, y)

    def cache_copies(t):
        rows = pl.ds(row_block(t) * 16, 16)
        return (
            pltpu.make_async_copy(k_in.at[rows], kbuf.at[t % RING], isem.at[0, t % RING]),
            pltpu.make_async_copy(v_in.at[rows], vbuf.at[t % RING], isem.at[1, t % RING]),
        )

    def cols(start, width):
        return pl.ds(pl.multiple_of(start, 128), width)

    wcp = [
        [
            pltpu.make_async_copy(wk.at[:, cols(core * 256, 256)], wbuf.at[0, :, pl.ds(0, 256)], wsem.at[0]),
            pltpu.make_async_copy(wv.at[:, cols(core * 256, 256)], wbuf.at[0, :, pl.ds(256, 256)], wsem.at[1]),
        ],
        [pltpu.make_async_copy(wq.at[:, cols(core * 1024, 512)], wbuf.at[1], wsem.at[2])],
        [pltpu.make_async_copy(wq.at[:, cols(core * 1024 + 512, 512)], wbuf.at[2], wsem.at[3])],
    ]
    ocp = [
        pltpu.make_async_copy(
            wo.at[:, pl.ds(512 * i, 512)], wbuf.at[i // 2, pl.ds(2048 * (i % 2), 2048)], wsem.at[4 + i]
        )
        for i in range(8)
    ]
    for group in wcp:
        for c in group:
            c.start()
    for c in cache_copies(0):
        c.start()

    n_s[...] = rms(x_ref[...].astype(F32), gain_ref).astype(BF16)
    ang = column(pos_v[...].astype(F32)) * freq_ref[...]
    lane = lax.broadcasted_iota(jnp.int32, (ROWS, HD), 1)
    even = (lane & 1) == 0
    cosr = jnp.cos(ang)
    sinr = jnp.sin(ang)
    sinr = jnp.where(even, -sinr, sinr)
    slotb[...] = (lax.broadcasted_iota(jnp.int32, (SLOTS * KVH, HD), 0) >> 2).astype(F32).astype(BF16)

    def rotate(y):
        swap = jnp.where(even, pltpu.roll(y, HD - 1, 1), pltpu.roll(y, 1, 1))
        return y * cosr + swap * sinr

    qcp = []
    for j in range(3):
        for c in wcp[j]:
            c.wait()
        y = jnp.dot(n_s[...], wbuf[j], preferred_element_type=F32)
        for t in range(1 + j, RING if j == 2 else 2 + j):
            for c in cache_copies(t):
                c.start()
        for hh in range(4):
            yh = y[:, hh * HD : (hh + 1) * HD]
            if j == 0 and hh < 2:
                kvraw[0, 2 * core + hh] = rotate(yh)
            elif j == 0:
                kvraw[1, 2 * core + hh - 2] = yh
            else:
                qraw[8 * core + (j - 1) * 4 + hh] = rotate(yh)
        if j == 0:
            pl.semaphore_wait(bar, 2)
            for i in range(PAIR):
                ref = kvraw.at[i, pl.ds(2 * core, 2)]
                qcp.append(rc(ref, ref, qsem.at[i], dev_c))
        else:
            ref = qraw.at[pl.ds(8 * core + (j - 1) * 4, 4)]
            qcp.append(rc(ref, ref, qsem.at[1 + j], dev_c))
            if j == 1:
                qcp[0].start()
                qcp[1].start()
                qcp[2].start()
            else:
                qcp[3].start()
    for c in qcp[:PAIR]:
        c.wait_recv()
    for i, (dup, out) in enumerate(((kdup, kn_out), (vdup, vn_out))):
        for h in range(KVH):
            v = kvraw[i, h]
            ofin[pl.ds(h, ROWS, stride=KVH), :] = v
            for rep in range(PAIR):
                dup[pl.ds(rep * KVH + h, ROWS, stride=8), :] = v
        out[...] = ofin[...].astype(BF16)
    for j, c in enumerate(qcp[PAIR:]):
        c.wait_recv()
        for h in range(QH):
            if h // KVH % PAIR == j:
                qf[pl.ds(h, ROWS, stride=QH), :] = qraw[h]

    col = lax.broadcasted_iota(jnp.int32, (QH, SLOTS * KVH), 1)
    hrow = lax.broadcasted_iota(jnp.int32, (QH, SLOTS * KVH), 0)
    slot_id = jnp.where((col & 3) == (hrow >> 2), col >> 2, jnp.int32(1 << 20))
    eye = lax.broadcasted_iota(jnp.int32, (128, 128), 0) == lax.broadcasted_iota(
        jnp.int32, (128, 128), 1
    )

    def merge(a, b, put, last):
        m1, m2 = a[M_AT, :], b[M_AT, :]
        l1, l2 = a[L_AT, :], b[L_AT, :]
        m = jnp.maximum(m1, m2)
        a1 = jnp.exp(m1 - m)
        a2 = jnp.exp(m2 - m)
        l = a1 * l1 + a2 * l2
        if last:
            a1 = a1 / l
            a2 = a2 / l
        for g in range(PAIR):
            rows = pl.ds(g * 128, 128)
            put(g, column(a1[g : g + 1]) * a[rows, :] + column(a2[g : g + 1]) * b[rows, :])
        return m, l

    def merge_into(dst, a, b):
        def put(g, v):
            dst[pl.ds(g * 128, 128), :] = v

        m, l = merge(a, b, put, False)
        dst[M_AT, :] = m
        dst[L_AT, :] = l

    pair = {
        "a": block_of(oc, ox, 0),
        "x": block_of(core, ox, 0),
        "b": block_of(oc, xi, 0),
        "own": block_of(core, xi, 0),
    }
    send_a = rc(o_s.at[pl.ds(pair["a"], 2)], rba, bsem.at[0], dev_c)
    send_b = rc(o_s.at[pl.ds(pair["b"], 2)], rbb, bsem.at[1], dev_c)
    send_x = [rc(ob.at[q], rbx.at[q], bsem.at[2 + q], dev_x) for q in range(PAIR)]

    def patched(dup, buf, t, b, row, lim):
        hit = slotb[...] == lax.broadcast(lim.astype(F32), (SLOTS * KVH, HD)).astype(BF16)
        d = dup[pl.ds(pl.multiple_of(row * 8, 8), 8), :]
        d = jnp.concatenate([d, d], axis=0).astype(BF16)
        d = jnp.concatenate([d] * 32, axis=0)
        return jnp.where(hit, d, buf[t % RING, b])

    def block(t, _):
        r = row_block(t)
        for c in cache_copies(t):
            c.wait()

        @pl.when(t == 2)
        def _():
            for c in ocp:
                c.start()

        for half in range(PAIR):
            sc, lims = [], []
            for b in range(8):
                row = r * 16 + half * 8 + b
                lim = pos_s[row] - sp * SLOTS
                lims.append(lim)
                q = qf[pl.ds(pl.multiple_of(row * QH, QH), QH), :].astype(BF16)
                sc.append(
                    lax.dot_general(
                        q, patched(kdup, kbuf, t, half * 8 + b, row, lim), (((1,), (1,)), ((), ())), preferred_element_type=F32
                    )
                )
            ms, ls = [], []
            for b in range(8):
                ok = slot_id <= lims[b]
                s = jnp.where(ok, sc[b] * (HD**-0.5), NEG)
                m = jnp.maximum(jnp.max(s, axis=-1, keepdims=True), NEG * 0.1)
                w = jnp.exp(s - m)
                ms.append(m)
                ls.append(jnp.sum(w, axis=-1, keepdims=True))
                v = patched(vdup, vbuf, t, half * 8 + b, r * 16 + half * 8 + b, lims[b])
                o = jnp.dot(w.astype(BF16), v, preferred_element_type=F32)
                o_s[r, pl.ds((half * 8 + b) * QH, QH), :] = o
            m = jnp.concatenate(ms, axis=0)
            l = jnp.concatenate(ls, axis=0)
            o_s[r, pl.ds(256 + half, 1), :] = jnp.sum(jnp.where(eye, m, 0.0), axis=0, keepdims=True)
            o_s[r, pl.ds(258 + half, 1), :] = jnp.sum(jnp.where(eye, l, 0.0), axis=0, keepdims=True)

        @pl.when(t == 1)
        def _():
            send_a.start()

        for q in range(PAIR):

            @pl.when(t == 2 + q)
            def _():
                if q == 0:
                    send_a.wait_recv()
                merge_into(ob.at[q], o_s.at[pair["x"] + q], rba.at[q])
                send_x[q].start()

        @pl.when(t == 5)
        def _():
            send_b.start()

        @pl.when(t < 8 - RING)
        def _():
            for c in cache_copies(t + RING):
                c.start()

        return 0

    lax.fori_loop(0, 8, block, 0)
    send_b.wait_recv()
    for q in range(PAIR):
        merge_into(ob.at[2 + q], o_s.at[pair["own"] + q], rbb.at[q])
    for q in range(PAIR):
        send_x[q].wait_recv()

        def put(g, v):
            ofin[pl.ds(q * 256 + g * 128, 128), :] = v

        merge(ob.at[2 + q], rbx.at[q], put, True)
    for h in range(QH):
        obf[:, h * HD : (h + 1) * HD] = ofin[pl.ds(h, 32, stride=QH), :].astype(BF16)

    for c in ocp:
        c.wait()
    for i in range(4):
        v = jnp.concatenate(
            [
                jnp.dot(obf[...], wbuf[i, 2048 * k : 2048 * (k + 1), :], preferred_element_type=F32)
                for k in range(PAIR)
            ],
            axis=1,
        )
        cs = pl.ds(i * 1024, 1024)
        own_out[:, cs] = jnp.where(yi == 0, v[:16], v[16:])
        oth_out[:, cs] = jnp.where(yi == 0, v[16:], v[:16])
    for c in qcp + send_x + [send_a, send_b]:
        c.wait_send()


def run_front(pos, x, gain, wq, wk, wv, wo, k_blk, v_blk):
    half_idx = np.arange(HD // 2, dtype=np.float32)
    inv = (1.0 / np.power(np.float32(ROPE_THETA), np.float32(2.0) * half_idx / np.float32(HD))).astype(np.float32)
    freq = jnp.asarray(np.repeat(inv, 2)[None, :])
    vm = pl.BlockSpec(memory_space=pltpu.VMEM)
    hbm = pl.BlockSpec(memory_space=pl.ANY)
    ring = pltpu.VMEM((RING, 16, SLOTS * KVH, HD), BF16)
    dup = jax.ShapeDtypeStruct((ROWS * 8, HD), F32)
    new = jax.ShapeDtypeStruct((ROWS * KVH, HD), BF16)
    rows = jax.ShapeDtypeStruct((16, DIM), F32)
    part = pltpu.VMEM((2, 264, 128), F32)
    return pl.pallas_call(
        front_kernel,
        name="front",
        out_shape=[new, new, dup, dup, rows, rows],
        in_specs=[pl.BlockSpec(memory_space=pltpu.SMEM), vm, vm, vm, vm] + [hbm] * 6,
        out_specs=[vm] * 6,
        scratch_shapes=[
            pltpu.VMEM((ROWS, DIM), BF16),
            pltpu.VMEM((4, DIM, 512), BF16),
            ring,
            ring,
            pltpu.VMEM((QH, ROWS, HD), F32),
            pltpu.VMEM((2, KVH, ROWS, HD), F32),
            pltpu.VMEM((ROWS * QH, HD), F32),
            pltpu.VMEM((SLOTS * KVH, HD), BF16),
            pltpu.VMEM((8, 264, 128), F32),
            part,
            part,
            part,
            pltpu.VMEM((4, 264, 128), F32),
            pltpu.VMEM((512, 128), F32),
            pltpu.VMEM((32, 2048), BF16),
            pltpu.SemaphoreType.DMA((12,)),
            pltpu.SemaphoreType.DMA((2, RING)),
            pltpu.SemaphoreType.DMA((4, 2)),
            pltpu.SemaphoreType.DMA((4, 2)),
        ],
        compiler_params=pltpu.CompilerParams(
            collective_id=1, has_side_effects=True, vmem_limit_bytes=60 * MIB
        ),
        cost_estimate=pl.CostEstimate(flops=4 * 10**9, bytes_accessed=63 * 10**6, transcendentals=10**6),
    )(
        pos, x, pos[None, :], freq, gain.reshape(32, 128), wq, wk, wv, wo,
        k_blk.reshape(ROWS, SLOTS * KVH, HD), v_blk.reshape(ROWS, SLOTS * KVH, HD),
    )


def write_kernel(
    pos_s, kdup_in, vdup_in, kn_in, vn_in, k_in, v_in,
    k_out, v_out, kn_out, vn_out, tok,
    kbuf, vbuf, kdup, vdup, kn, vn, isem, osem, ssem, nsem,
):
    sp = lax.axis_index("sp")

    def copies_in(i, s):
        rows = pl.ds(i * WROWS, WROWS)
        return (
            pltpu.make_async_copy(k_in.at[rows], kbuf.at[s], isem.at[0, s]),
            pltpu.make_async_copy(v_in.at[rows], vbuf.at[s], isem.at[1, s]),
        )

    def copies_out(i, s):
        rows = pl.ds(i * WROWS, WROWS)
        return (
            pltpu.make_async_copy(kbuf.at[s], k_out.at[rows], osem.at[0, s]),
            pltpu.make_async_copy(vbuf.at[s], v_out.at[rows], osem.at[1, s]),
        )

    small = [
        pltpu.make_async_copy(a, b, ssem.at[i])
        for i, (a, b) in enumerate(((kdup_in, kdup), (vdup_in, vdup), (kn_in, kn), (vn_in, vn)))
    ]
    new = [
        pltpu.make_async_copy(a, b, nsem.at[i]) for i, (a, b) in enumerate(((kn, kn_out), (vn, vn_out)))
    ]
    for c in small:
        c.start()
    for i in range(WSTEPS):
        for c in copies_in(i, i):
            c.start()
    tok[...] = jnp.zeros_like(tok)
    for c in small:
        c.wait()
    for c in new:
        c.start()
    r16 = lax.broadcasted_iota(jnp.int32, (16, HD), 0) >> 2

    def block(r, _):
        s = r
        for c in copies_in(r, s):
            c.wait()
        for b in range(WROWS):
            row = r * WROWS + b
            lim = pos_s[row] - sp * SLOTS
            cl = jnp.clip(lim, 0, SLOTS - 1)
            at = pl.ds(pl.multiple_of((cl >> 2) * 16, 16), 16)
            hit = r16 == jnp.where(lim == cl, cl & 3, -1)
            of_row = pl.ds(pl.multiple_of(row * 8, 8), 8)
            for dup, buf in ((kdup, kbuf), (vdup, vbuf)):
                d = dup[of_row, :]
                d = jnp.concatenate([d, d], axis=0).astype(BF16)
                buf[s, b, at, :] = jnp.where(hit, d, buf[s, b, at, :])
        return 0

    lax.fori_loop(0, WSTEPS, block, 0)
    for i in range(WSTEPS):
        for c in copies_out(i, i):
            c.start()
    for i in range(WSTEPS):
        for c in copies_out(i, i):
            c.wait()
    for c in new:
        c.wait()


def run_write(pos, kdup, vdup, kn, vn, k_blk, v_blk):
    vm = pl.BlockSpec(memory_space=pltpu.VMEM)
    hbm = pl.BlockSpec(memory_space=pl.ANY)
    cache = jax.ShapeDtypeStruct((ROWS, SLOTS * KVH, HD), BF16)
    new = jax.ShapeDtypeStruct((ROWS * KVH, HD), BF16)
    dup = pltpu.VMEM((ROWS * 8, HD), F32)
    small = pltpu.VMEM((ROWS * KVH, HD), BF16)
    ring = pltpu.VMEM((WSTEPS, WROWS, SLOTS * KVH, HD), BF16)
    return pl.pallas_call(
        write_kernel,
        name="write",
        out_shape=[cache, cache, new, new, jax.ShapeDtypeStruct((8, 128), F32)],
        in_specs=[pl.BlockSpec(memory_space=pltpu.SMEM)] + [hbm] * 6,
        out_specs=[hbm] * 4 + [vm],
        scratch_shapes=[
            ring,
            ring,
            dup,
            dup,
            small,
            small,
            pltpu.SemaphoreType.DMA((2, WSTEPS)),
            pltpu.SemaphoreType.DMA((2, WSTEPS)),
            pltpu.SemaphoreType.DMA((4,)),
            pltpu.SemaphoreType.DMA((2,)),
        ],
        compiler_params=pltpu.CompilerParams(vmem_limit_bytes=VMEM_MAX),
        cost_estimate=pl.CostEstimate(flops=5 * 10**9, bytes_accessed=67 * 10**6, transcendentals=0),
    )(
        pos, kdup, vdup, kn, vn,
        k_blk.reshape(ROWS, SLOTS * KVH, HD), v_blk.reshape(ROWS, SLOTS * KVH, HD),
    )


WROWS = 16
WSTEPS = ROWS // WROWS
NG = 4
GW = DIM // NG
TAIL_VMEM = 62 * MIB + MIB // 2
NC = 4
CW = DIM // NC
HC = CW // 2


def tail_kernel(
    own_in, oth_in, x_in, gain_ref, wg, wu, wd, tok,
    out_ref,
    wd_v, wg_v, wu_v, hs, xs, gat, nbf, act,
    part, rd, r1, r2, gat2, wsem, gsem, fsem,
):
    del tok
    sp, yi, core, xi, oc, ox, dev_c, dev_x, dev_y = place()
    oy = 1 - yi
    me, me_x, me_y, me_xy = (block_of(core, a, b) for a, b in ((xi, yi), (ox, yi), (xi, oy), (ox, oy)))

    bar = pltpu.get_barrier_semaphore()
    for dev in (dev_c, dev_x, dev_y):
        pl.semaphore_signal(bar, inc=1, device_id=dev, device_id_type=MESH)

    hcols = pl.ds(pl.multiple_of(sp * HSL, 128), HSL)
    cx = pltpu.make_async_copy(x_in.at[me], xs, wsem.at[0])
    cx.start()
    cup = []
    for j in range(NG):
        ks = pl.ds(j * GW, GW)
        cup.append(
            [
                pltpu.make_async_copy(wg.at[ks, hcols], wg_v.at[ks], wsem.at[2 + 2 * j]),
                pltpu.make_async_copy(wu.at[ks, hcols], wu_v.at[ks], wsem.at[3 + 2 * j]),
            ]
        )
        for c in cup[j]:
            c.start()
    cwd = pltpu.make_async_copy(wd.at[hcols], wd_v, wsem.at[1])
    cwd.start()
    cx.wait()
    hs[...] = xs[...].astype(F32) + (own_in[...] + oth_in[...])
    gat[me] = rms(hs[...], gain_ref).astype(BF16).astype(F32)
    pl.semaphore_wait(bar, 3)

    def gather0(buf, c0, w, sems):
        cs = pl.ds(c0, w)
        out = []
        for k, dev in ((0, dev_x), (1, dev_y), (2, dev_c)):
            c = rc(buf.at[me, :, cs], buf.at[me, :, cs], sems.at[k], dev)
            c.start()
            out.append(c)
        return out

    def gather1(buf, c0, w, sems, cps):
        lo, hi, cs = pl.ds(c0, w // 2), pl.ds(c0 + w // 2, w // 2), pl.ds(c0, w)
        cps[0].wait_recv()
        a = rc(buf.at[me_x, :, lo], buf.at[me_x, :, lo], sems.at[3], dev_y)
        a.start()
        b = rc(buf.at[me_x, :, cs], buf.at[me_x, :, cs], sems.at[4], dev_c)
        b.start()
        cps[1].wait_recv()
        c = rc(buf.at[me_y, :, hi], buf.at[me_y, :, hi], sems.at[5], dev_x)
        c.start()
        d = rc(buf.at[me_y, :, cs], buf.at[me_y, :, cs], sems.at[6], dev_c)
        d.start()
        return [a, b, c, d]

    def gather2(buf, c0, w, sems, cps):
        cs = pl.ds(c0, w)
        cps[0].wait_recv()
        cps[2].wait_recv()
        c = rc(buf.at[me_xy, :, cs], buf.at[me_xy, :, cs], sems.at[7], dev_c)
        c.start()
        return [c]

    g0 = [gather0(gat, j * GW, GW, gsem.at[j]) for j in range(NG)]
    g1 = [gather1(gat, j * GW, GW, gsem.at[j], g0[j]) for j in range(NG)]
    g2 = []

    def up(j):
        for c in (g0[j][2], g1[j][1], g1[j][3], g2[j][0]):
            c.wait_recv()
        ks = pl.ds(j * GW, GW)
        for r in range(8):
            nbf[pl.ds(r * 16, 16), :] = gat[r, :, ks].astype(BF16)

        for c in cup[j]:
            c.wait()
        for w, base in ((wg_v, 0), (wu_v, HSL)):
            v = jnp.dot(nbf[...], w[ks, :], preferred_element_type=F32).reshape(8, 16, HSL)
            cols = pl.ds(base, HSL)
            part[:, :, cols] = v if j == 0 else part[:, :, cols] + v

    for j in range(NG):
        g2.append(gather2(gat, j * GW, GW, gsem.at[j], g1[j]))
        if j:
            up(j - 1)
    up(NG - 1)

    def gate(i, _):
        cols = pl.ds(pl.multiple_of(i * 256, 256), 256)
        g = part[:, :, cols].reshape(ROWS, 256)
        u = part[:, :, pl.ds(pl.multiple_of(HSL + i * 256, 256), 256)].reshape(ROWS, 256)
        act[:, cols] = (jax.nn.silu(g) * u).astype(BF16)
        return 0

    lax.fori_loop(0, HSL // 256, gate, 0)
    cwd.wait()

    state = [dict() for _ in range(NC)]

    def s0(j):
        cs = pl.ds(j * CW, CW)
        v = jnp.dot(act[...], wd_v[:, cs], preferred_element_type=F32)
        part[:, :, cs] = v.reshape(8, 16, CW)
        c = rc(part.at[pl.ds(4 * oc, 4), :, cs], rd.at[:, :, cs], fsem.at[j, 8], dev_c)
        c.start()
        state[j]["d"] = c

    def s1(j):
        cs = pl.ds(j * CW, CW)
        state[j]["d"].wait()
        mine = pl.ds(4 * core, 4)
        rd[:, :, cs] = part[mine, :, cs] + rd[:, :, cs]
        if j % 2 == 0:
            c = [rc(rd.at[pl.ds(2 * ox, 2), :, cs], r1.at[:, :, cs], fsem.at[j, 9], dev_x)]
        else:
            c = [
                rc(rd.at[2 * i + oy, :, cs], r1.at[i, :, cs], fsem.at[j, 9 + i], dev_y)
                for i in range(PAIR)
            ]
        for k in c:
            k.start()
        state[j]["r"] = c

    def s2(j):
        cs = pl.ds(j * CW, CW)
        for k in state[j]["r"]:
            k.wait_recv()
        if j % 2 == 0:
            for i in range(PAIR):
                r1[i, :, cs] = r1[i, :, cs] + rd[2 * xi + i, :, cs]
            c = rc(r1.at[oy, :, cs], r2.at[:, cs], fsem.at[j, 11], dev_y)
        else:
            for i in range(PAIR):
                r1[i, :, cs] = r1[i, :, cs] + rd[2 * i + yi, :, cs]
            c = rc(r1.at[ox, :, cs], r2.at[:, cs], fsem.at[j, 11], dev_x)
        c.start()
        state[j]["r2"] = c

    def s3(j):
        cs = pl.ds(j * CW, CW)
        state[j]["r2"].wait_recv()
        own = r1[yi, :, cs] if j % 2 == 0 else r1[xi, :, cs]
        y = hs[:, cs] + (own + r2[:, cs])
        gat2[me, :, cs] = y.astype(BF16).astype(F32)
        state[j]["g0"] = gather0(gat2, j * CW, CW, fsem.at[j])

    def s4(j):
        state[j]["g1"] = gather1(gat2, j * CW, CW, fsem.at[j], state[j]["g0"])

    def s5(j):
        state[j]["g2"] = gather2(gat2, j * CW, CW, fsem.at[j], state[j]["g1"])

    def s6(j):
        cs = pl.ds(j * CW, CW)
        st = state[j]
        for c in (st["g0"][2], st["g1"][1], st["g1"][3], st["g2"][0]):
            c.wait_recv()
        out_ref[:, :, cs] = gat2[:, :, cs].astype(BF16)

    for t in range(NC + 1):
        if t < NC:
            s0(t)
        if t:
            s1(t - 1)
    for stage in (s2, s3, s4, s5, s6):
        for j in range(NC):
            stage(j)

    for c in sum(g0 + g1 + g2, []):
        c.wait_send()
    for st in state:
        for c in st["r"] + [st["r2"]] + st["g0"] + st["g1"] + st["g2"]:
            c.wait_send()


def run_tail(own, oth, x, gain, wg, wu, wd, tok):
    vm = pl.BlockSpec(memory_space=pltpu.VMEM)
    hbm = pl.BlockSpec(memory_space=pl.ANY)
    return pl.pallas_call(
        tail_kernel,
        name="tail",
        out_shape=pltpu.VMEM((8, 16, DIM), BF16),
        in_specs=[vm, vm, hbm, vm, hbm, hbm, hbm, hbm],
        out_specs=vm,
        scratch_shapes=[
            pltpu.VMEM((HSL, DIM), BF16),
            pltpu.VMEM((DIM, HSL), BF16),
            pltpu.VMEM((DIM, HSL), BF16),
            pltpu.VMEM((16, DIM), F32),
            pltpu.VMEM((16, DIM), BF16),
            pltpu.VMEM((8, 16, DIM), F32),
            pltpu.VMEM((ROWS, GW), BF16),
            pltpu.VMEM((ROWS, HSL), BF16),
            pltpu.VMEM((8, 16, DIM), F32),
            pltpu.VMEM((4, 16, DIM), F32),
            pltpu.VMEM((2, 16, DIM), F32),
            pltpu.VMEM((16, DIM), F32),
            pltpu.VMEM((8, 16, DIM), F32),
            pltpu.SemaphoreType.DMA((2 + 2 * NG,)),
            pltpu.SemaphoreType.DMA((NG, 8, 2)),
            pltpu.SemaphoreType.DMA((NC, 12, 2)),
        ],
        compiler_params=pltpu.CompilerParams(
            collective_id=0, has_side_effects=True, vmem_limit_bytes=TAIL_VMEM
        ),
        cost_estimate=pl.CostEstimate(flops=6 * 10**9, bytes_accessed=62 * 10**6, transcendentals=10**6),
    )(own, oth, x.reshape(8, 16, DIM), gain.reshape(32, 128), wg, wu, wd, tok)


def solution(mesh):
    def local_step(layer_in, new_pos, k_blk, v_blk, attn_gain, w_query, w_key, w_value, w_out, mlp_gain, w_gate, w_up, w_down):
        kn, vn, kdup, vdup, own, oth = run_front(
            new_pos, layer_in, attn_gain, w_query, w_key, w_value, w_out, k_blk, v_blk
        )
        oth = lax.ppermute(oth, 'tp', [(0, 1), (1, 0)])
        k_upd, v_upd, k_new, v_new, tok = run_write(new_pos, kdup, vdup, kn, vn, k_blk, v_blk)
        y = run_tail(own, oth, layer_in, mlp_gain, w_gate, w_up, w_down, tok)
        shape = (ROWS, SLOTS, KVH, HD)
        new = (ROWS, KVH, HD)
        return y.reshape(ROWS, DIM), k_upd.reshape(shape), v_upd.reshape(shape), k_new.reshape(new), v_new.reshape(new)

    cache_spec = P('dp', 'sp', 'tp', None)
    new_spec = P('dp', 'tp', None)
    in_specs = (P('dp', None), P('dp'), cache_spec, cache_spec, P(None), P(None, 'tp'), P(None, 'tp'), P(None, 'tp'), P('tp', None), P(None), P(None, 'tp'), P(None, 'tp'), P('tp', None))
    out_specs = (P('dp', None), cache_spec, cache_spec, new_spec, new_spec)
    return jax.shard_map(local_step, mesh=mesh, in_specs=in_specs, out_specs=out_specs, check_vma=False)
```
